512 devices in a mesh: groups: 2 (over y), branch: 2 (over core), tok: 128 (over x, z).
Axes of the slice: x: 8, y: 2, z: 16, core: 2. Of those that a mesh axis runs over, the one named last changes fastest.
The devices are a block of a 8x8x16 slice.
Arguments:
- queries: bfloat16 [8192, 4096], P(('groups', 'tok')), parts along dimension 0, may hold values from -8 to 8
- keys: bfloat16 [8192, 4096], P(('groups', 'tok')), parts along dimension 0, may hold values from -8 to 8
- values: bfloat16 [8192, 4096], P(('groups', 'tok')), parts along dimension 0, may hold values from -6 to 6
- keyboard: int32 [16], P('groups'), parts along dimension 0, may hold values from 0 to 15
- mouse: int32 [16], P('groups'), parts along dimension 0, may hold values from 0 to 31
- key_table: bfloat16 [16, 2, 4096], replicated, may hold values from -3 to 3
- mouse_table: bfloat16 [32, 2, 4096], replicated, may hold values from -3 to 3
- guidance: float32 [4], replicated, may hold values from 0.5 to 1.5
- out_weight: bfloat16 [4096, 64], replicated, may hold values from -0.09375 to 0.09375
- latent: float32 [8192, 64], P(('groups', 'tok')), parts along dimension 0, may hold values from -6 to 6
- conv_in: bfloat16 [3, 3, 16, 384], replicated, may hold values from -0.5 to 0.5
- gain: float32 [384], replicated, may hold values from 0.5 to 1.5
- conv_out: bfloat16 [3, 3, 384, 3], replicated, may hold values from -0.109375 to 0.109375
Outputs:
- velocity: float32 [8192, 64], P(('groups', 'tok')), parts along dimension 0
- frames_rgb: float32 [3, 512, 64], P(None, ('groups', 'tok')), parts along dimension 1
The draws below stay inside these ranges and needn't reach their ends.
There are 2 independent parts, one for each index of `groups`. The reference program is written for one: setup_inputs(seed, part) draws one part's arguments, and reference() takes and returns one part's arrays. A program takes and returns all parts, laid end to end along the dimension named above; an argument that names none is the same for every part. Nothing has to cross between parts.
All inputs are finite; a program needn't handle non-finite values.
Results may differ from the reference program's by a relative error of at most 0.012.
Values may be sent and summed in bfloat16 or wider, within the bound.
No kernel may reach another device: no remote copies, remote signals or barrier semaphores. Data moves between devices by JAX's collectives and lax.ppermute only.
A program may use at most 64 MiB of HBM per device.

```python
import jax
import jax.numpy as jnp
from jax import lax

HEAD_DIM = 128
HEADS = 32
D = 4096
TOK_DEV = 32
TOKENS = 4096
FRAMES = 8
LAT_CH = 16
PATCH_CH = 64
DEC = 384
KEYS = 16
MOUSE = 32
BRANCHES = 4
N_TOK = 128


def base_field(key):
    field = 1.5 * jax.random.normal(jax.random.fold_in(key, 6), (TOKENS, D))
    return jnp.clip(field, -8.0, 8.0)


def draw_queries(key, part):
    field = base_field(jax.random.fold_in(key, 101))
    return field.astype(jnp.bfloat16)


def draw_keys(key, part):
    field = base_field(jax.random.fold_in(key, 202))
    return field.astype(jnp.bfloat16)


def with_ends(result, own_key, smallest, top_value):
    dims = result.shape
    index_at = [jax.random.randint(jax.random.fold_in(own_key, axis), (), 0, dims[axis]) for axis in range(len(dims))]
    result = result.at[tuple(index_at)].set(smallest)
    longest = dims.index(max(dims))
    index_at[longest] = (index_at[longest] + 1) % dims[longest]
    return result.at[tuple(index_at)].set(top_value)


def levels(key, extent, cuts, low, high):
    factor_of, own = 1.0, jax.random.fold_in(key, 6)
    for axis_at, parts in cuts:
        heights = jnp.exp(jax.random.uniform(jax.random.fold_in(own, axis_at), (parts,), jnp.float32, low / len(cuts), high / len(cuts)))
        factor_of = factor_of * jnp.repeat(heights, extent[axis_at] // parts).reshape([-1 if axis == axis_at else 1 for axis in range(len(extent))])
    return factor_of


def scatter_about(key, extent, width, bound, shards=(), kind=jnp.bfloat16):
    drawn = jax.random.normal(key, extent, jnp.float32) * width
    if len(shards) > 0:
        drawn = levels(key, extent, shards, -0.22, 0.18) * drawn
    return jnp.clip(drawn, min=-bound, max=bound).astype(kind)


def setup_inputs(seed: int = 0, part: int = 0) -> dict:
    key_list = jax.random.split(jax.random.key(seed), 14)
    part_splits = jax.random.split(jax.random.fold_in(key_list[13], part), 14)
    return {
        "queries": draw_queries(jax.random.fold_in(jax.random.fold_in(key_list[13], part), 71), part),
        "keys": draw_keys(jax.random.fold_in(jax.random.fold_in(key_list[13], part), 71), part),
        "values": scatter_about(part_splits[2], (TOKENS, D), 1.0, 6.0, ((0, 128),)),
        "keyboard": with_ends(jax.random.randint(part_splits[3], (FRAMES,), 0, KEYS), jax.random.fold_in(part_splits[3], 1), 0, KEYS - 1).astype(jnp.int32),
        "mouse": with_ends(jax.random.randint(part_splits[4], (FRAMES,), 0, MOUSE), jax.random.fold_in(part_splits[4], 1), 0, MOUSE - 1).astype(jnp.int32),
        "key_table": scatter_about(key_list[5], (KEYS, 2, D), 0.5, 3.0),
        "mouse_table": scatter_about(key_list[6], (MOUSE, 2, D), 0.5, 3.0),
        "guidance": jnp.clip(jax.random.uniform(key_list[7], (BRANCHES,), jnp.float32, 0.5, 1.5), 0.5, 1.5),
        "out_weight": scatter_about(key_list[8], (D, PATCH_CH), D ** -0.5, 0.09375),
        "latent": scatter_about(part_splits[9], (TOKENS, PATCH_CH), 1.0, 6.0, ((0, 128),), jnp.float32),
        "conv_in": scatter_about(key_list[10], (3, 3, LAT_CH, DEC), (9 * LAT_CH) ** -0.5, 0.5),
        "gain": jnp.clip(1.0 + 0.1 * jax.random.normal(key_list[11], (DEC,), jnp.float32), 0.5, 1.5),
        "conv_out": scatter_about(key_list[12], (3, 3, DEC, 3), (9 * DEC) ** -0.5, 0.109375),
    }


step_size = 0.25
norm_eps = 1e-06
branch_flags = ((1.0, 1.0), (0.0, 1.0), (1.0, 0.0), (0.0, 0.0))

def action_terms(keyboard, mouse, key_table, mouse_table, flag_key, flag_mouse):
    pick_key = (keyboard[:, None] == jnp.arange(KEYS, dtype=jnp.int32)[None, :]).astype(jnp.float32)
    pick_mouse = (mouse[:, None] == jnp.arange(MOUSE, dtype=jnp.int32)[None, :]).astype(jnp.float32)
    rows_key = jnp.einsum('fk,kcd->fcd', pick_key, key_table.astype(jnp.float32))
    rows_mouse = jnp.einsum('fk,kcd->fcd', pick_mouse, mouse_table.astype(jnp.float32))
    return flag_key * rows_key + flag_mouse * rows_mouse

def convolve(padded, weight):
    rows = padded.shape[1] - 2
    cols = padded.shape[2] - 2
    total = jnp.zeros((padded.shape[0], rows, cols, weight.shape[-1]), jnp.float32)
    for first in range(3):
        for second in range(3):
            window = padded[:, first:first + rows, second:second + cols, :].astype(jnp.float32)
            total = total + jnp.einsum('frci,io->frco', window, weight[first, second].astype(jnp.float32))
    return total

def reference(queries, keys, values, keyboard, mouse, key_table, mouse_table, guidance, out_weight, latent, conv_in, gain, conv_out):
    frame_tok = TOKENS // FRAMES
    terms = jnp.stack([action_terms(keyboard, mouse, key_table, mouse_table, branch_flags[b][0], branch_flags[b][1]) for b in range(BRANCHES)])
    key_bias = terms[:, :, 0].astype(jnp.bfloat16)
    value_term = terms[:, :, 1]
    key_bias = key_bias.reshape(BRANCHES, FRAMES, HEADS, HEAD_DIM).transpose(2, 0, 1, 3)
    value_term = value_term.reshape(BRANCHES, FRAMES, HEADS, HEAD_DIM).transpose(2, 0, 1, 3)
    head_queries = queries.reshape(TOKENS, HEADS, HEAD_DIM).transpose(1, 0, 2)
    head_keys = keys.reshape(TOKENS, HEADS, HEAD_DIM).transpose(1, 0, 2)
    head_values = values.reshape(TOKENS, HEADS, HEAD_DIM).transpose(1, 0, 2)

    def one_head(inputs):
        head_q, head_k, head_v, head_bias, head_term = inputs
        base = jnp.dot(head_q, head_k.T, preferred_element_type=jnp.float32)
        grouped = base.reshape(TOKENS, FRAMES, frame_tok)
        combined = jnp.zeros((TOKENS, HEAD_DIM), jnp.float32)
        for branch in range(BRANCHES):
            frame_scores = jnp.dot(head_q, head_bias[branch].T, preferred_element_type=jnp.float32)
            scores = (grouped + frame_scores[:, :, None]).reshape(TOKENS, TOKENS) * HEAD_DIM ** (-0.5)
            top = lax.optimization_barrier(jnp.max(scores, axis=-1, keepdims=True))
            raised = jnp.exp(scores - top)
            total = lax.optimization_barrier(jnp.sum(raised, axis=-1))
            shifted = head_v.astype(jnp.float32).reshape(FRAMES, frame_tok, HEAD_DIM) + head_term[branch][:, None, :]
            shifted = shifted.reshape(TOKENS, HEAD_DIM).astype(jnp.bfloat16)
            summed = jnp.dot(raised.astype(jnp.bfloat16), shifted, preferred_element_type=jnp.float32)
            attended = (summed / total[:, None]).astype(jnp.bfloat16)
            combined = combined + guidance[branch] * attended.astype(jnp.float32)
        return combined
    per_head = lax.map(one_head, (head_queries, head_keys, head_values, key_bias, value_term))
    combined = per_head.transpose(1, 0, 2).reshape(TOKENS, HEADS * HEAD_DIM).astype(jnp.bfloat16)
    velocity = jnp.dot(combined, out_weight, preferred_element_type=jnp.float32)
    stepped = latent - step_size * velocity
    patch_rows = N_TOK // FRAMES
    grid = stepped.reshape(FRAMES, patch_rows, TOK_DEV, 2, 2, LAT_CH).transpose(0, 1, 3, 2, 4, 5)
    grid = grid.reshape(1, FRAMES * 2 * patch_rows, 2 * TOK_DEV, LAT_CH).astype(jnp.bfloat16)
    padded = jnp.pad(grid, ((0, 0), (1, 1), (1, 1), (0, 0)))
    features = convolve(padded, conv_in)
    scaled = features * lax.rsqrt(lax.optimization_barrier(jnp.mean(features * features, axis=-1, keepdims=True)) + norm_eps) * gain
    normed = jax.nn.silu(scaled).astype(jnp.bfloat16)
    colours = convolve(jnp.pad(normed, ((0, 0), (1, 1), (1, 1), (0, 0))), conv_out)
    frames_rgb = colours.transpose(3, 0, 1, 2).reshape(3, FRAMES * 2 * patch_rows, 2 * TOK_DEV)
    return (velocity, frames_rgb)
```

```python
import functools
import math

import jax
import jax.numpy as jnp
from jax import lax
from jax.experimental import pallas as pl
from jax.experimental.pallas import tpu as pltpu
from jax.sharding import Mesh
from jax.sharding import PartitionSpec as P

HEAD_DIM = 128

step_size = 0.25
norm_eps = 1e-06
TO_EXP2 = HEAD_DIM ** (-0.5) / math.log(2.0)
BF = jnp.bfloat16
F32 = jnp.float32


def dot(a, b, dims, **kw):
    return lax.dot_general(a, b, (dims, ((), ())), preferred_element_type=F32, **kw)


def pack_kernel(core_ref, q_ref, k_ref, v_ref, w_ref, out_ref):
    sets, _, hd = out_ref.shape
    rows = q_ref.shape[0]
    half = rows // 2
    for z in range(sets):
        cols = slice(z * hd, (z + 1) * hd)
        out_ref[z, 0:rows, :] = q_ref[:, cols]
        out_ref[z, rows : 2 * rows, :] = k_ref[:, cols]
        projected = dot(v_ref[:, cols], w_ref[cols, :], ((1,), (0,))).astype(BF)
        out_ref[z, 2 * rows :, :] = jnp.concatenate([projected[:half], projected[half:]], axis=1)


def pack(core, queries, keys, values, out_weight, sets):
    rows = queries.shape[0]
    cols = sets * HEAD_DIM
    outs = out_weight.shape[1]
    block = pl.BlockSpec((rows, cols), lambda i, c: (0, c[0]))
    return pl.pallas_call(
        pack_kernel,
        grid_spec=pltpu.PrefetchScalarGridSpec(
            num_scalar_prefetch=1,
            grid=(1,),
            in_specs=[block, block, block, pl.BlockSpec((cols, outs), lambda i, c: (c[0], 0))],
            out_specs=pl.BlockSpec((sets, 2 * rows + rows // 2, HEAD_DIM), lambda i, c: (0, 0, 0)),
        ),
        out_shape=jax.ShapeDtypeStruct((sets, 2 * rows + rows // 2, HEAD_DIM), BF),
        name="pack",
    )(core[None], queries, keys, values, out_weight)


def terms_kernel(kb_ref, ms_ref, head_ref, key_ref, mouse_ref, w_ref, bias_ref, term_ref):
    frames = term_ref.shape[0] // 2
    rows_key = jnp.concatenate([key_ref[pl.ds(kb_ref[j], 1)] for j in range(frames)], axis=0)
    rows_mouse = jnp.concatenate([mouse_ref[pl.ds(ms_ref[j], 1)] for j in range(frames)], axis=0)
    rows_key = rows_key.astype(F32)
    rows_mouse = rows_mouse.astype(F32)
    bias_key, bias_mouse = rows_key[:, 0, :], rows_mouse[:, 0, :]
    bias = [bias_key + bias_mouse, bias_mouse, bias_key, jnp.zeros_like(bias_key)]
    bias_ref[...] = jnp.concatenate(bias, axis=0).astype(BF)
    terms = jnp.concatenate([rows_key[:, 1, :], rows_mouse[:, 1, :]], axis=0).astype(BF)
    term_ref[...] = dot(terms, w_ref[...], ((1,), (0,)))


def action_terms(head, kb, ms, key_table, mouse_table, out_weight):
    frames = kb.shape[0]
    outs = out_weight.shape[1]
    return pl.pallas_call(
        terms_kernel,
        grid_spec=pltpu.PrefetchScalarGridSpec(
            num_scalar_prefetch=3,
            grid=(1,),
            in_specs=[
                pl.BlockSpec(key_table.shape[:2] + (HEAD_DIM,), lambda i, a, b, h: (0, 0, h[0])),
                pl.BlockSpec(mouse_table.shape[:2] + (HEAD_DIM,), lambda i, a, b, h: (0, 0, h[0])),
                pl.BlockSpec((HEAD_DIM, outs), lambda i, a, b, h: (h[0], 0)),
            ],
            out_specs=[
                pl.BlockSpec((4 * frames, HEAD_DIM), lambda i, a, b, h: (0, 0)),
                pl.BlockSpec((2 * frames, outs), lambda i, a, b, h: (0, 0)),
            ],
        ),
        out_shape=[
            jax.ShapeDtypeStruct((4 * frames, HEAD_DIM), BF),
            jax.ShapeDtypeStruct((2 * frames, outs), F32),
        ],
        name="terms",
    )(kb, ms, head[None], key_table, mouse_table, out_weight)


def frame_kernel(rows, at, own_ref, *refs):
    kv_refs, (sum_ref, stat_ref) = refs[:-2], refs[-2:]
    sets, _, hd = own_ref.shape
    half = rows // 2
    outs = sum_ref.shape[0]
    query = own_ref[:, 0:rows, :].reshape(sets * rows, hd)

    def gathered(first, last):
        parts = [r[:, first:last, :].reshape(-1, hd) for r in kv_refs]
        return parts[0] if len(parts) == 1 else jnp.concatenate(parts, axis=0)

    key_low = gathered(at, at + half)
    key_high = gathered(at + half, at + rows)
    both = gathered(at + rows, at + rows + half)
    score_low = dot(key_low, query, ((1,), (1,)))
    score_high = dot(key_high, query, ((1,), (1,)))
    top = jnp.maximum(
        jnp.max(score_low, axis=0, keepdims=True), jnp.max(score_high, axis=0, keepdims=True)
    )
    raised_low = jnp.exp2((score_low - top) * TO_EXP2)
    raised_high = jnp.exp2((score_high - top) * TO_EXP2)
    total = jnp.sum(raised_low, axis=0, keepdims=True) + jnp.sum(raised_high, axis=0, keepdims=True)
    summed = dot(both[:, :outs], raised_low.astype(BF), ((0,), (0,)))
    summed = summed + dot(both[:, outs:], raised_high.astype(BF), ((0,), (0,)))
    sum_ref[...] = summed
    stat_ref[0:1, :] = top
    stat_ref[1:2, :] = total


def frame_attention(own, pieces, rows, at, outs):
    tokens = own.shape[0] * rows
    flops = 2 * tokens * tokens * (HEAD_DIM + outs)
    return pl.pallas_call(
        functools.partial(frame_kernel, rows, at),
        out_shape=[
            jax.ShapeDtypeStruct((outs, tokens), F32),
            jax.ShapeDtypeStruct((2, tokens), F32),
        ],
        cost_estimate=pl.CostEstimate(
            flops=flops, transcendentals=tokens * tokens, bytes_accessed=1 << 20
        ),
        name="frame",
    )(own, *pieces)


def guide_kernel(rows, count, guide_ref, own_ref, bias_ref, term_ref, *refs):
    sum_refs, stat_refs, out_ref = refs[:count], refs[count : 2 * count], refs[-1]
    sets, _, hd = own_ref.shape
    half = rows // 2
    query = own_ref[:, 0:rows, :].reshape(sets * rows, hd)
    shift = dot(bias_ref[...], query, ((1,), (1,)))
    tops = jnp.concatenate([r[0:1, :] for r in stat_refs], axis=0)
    totals = jnp.concatenate([r[1:2, :] for r in stat_refs], axis=0)
    parts = []
    for b in range(4):
        height = (tops + shift[b * count : (b + 1) * count]) * TO_EXP2
        factor = jnp.exp2(height - jnp.max(height, axis=0, keepdims=True))
        total = jnp.sum(factor * totals, axis=0, keepdims=True)
        parts.append(factor * (guide_ref[b] / total))
    mix = (parts[0] + parts[1]) + (parts[2] + parts[3])
    loads = jnp.concatenate(
        [(parts[0] + parts[2]) * totals, (parts[0] + parts[1]) * totals], axis=0
    )
    result = dot(term_ref[...], loads, ((0,), (0,)), precision=lax.Precision.HIGHEST)
    for j in range(count):
        result = result + mix[j : j + 1, :] * sum_refs[j][...]
    by_token = jnp.transpose(result).reshape(sets, rows, -1)
    out_ref[...] = jnp.concatenate([by_token[:, :half], by_token[:, half:]], axis=2).astype(BF)


def guide(guidance, own, bias, term, sums, stats, rows, outs):
    sets = own.shape[0]
    count = len(sums)
    vmem = pl.BlockSpec(memory_space=pltpu.VMEM)
    return pl.pallas_call(
        functools.partial(guide_kernel, rows, count),
        in_specs=[pl.BlockSpec(memory_space=pltpu.SMEM)] + [vmem] * (3 + 2 * count),
        out_specs=vmem,
        out_shape=jax.ShapeDtypeStruct((sets, rows // 2, 2 * outs), BF),
        name="guide",
    )(guidance, own, bias, term, *sums, *stats)


def ring(count, steps):
    return [(i, (i + steps) % count) for i in range(count)]


def clear_rows(array, depth, top_edge, bottom_edge):
    height = array.shape[0]
    place = jnp.arange(height, dtype=jnp.int32)
    drop = (place < depth) & top_edge | (place >= height - depth) & bottom_edge
    return jnp.where(drop[:, None, None], jnp.zeros_like(array), array)


def convolve(array, weight):
    rows = array.shape[0] - 2
    cols = array.shape[1]
    padded = jnp.pad(array, ((0, 0), (1, 1), (0, 0)))
    total = jnp.zeros((rows, cols, weight.shape[-1]), F32)
    for first in range(3):
        for second in range(3):
            window = padded[first : first + rows, second : second + cols, :]
            total = total + jnp.einsum(
                "rci,io->rco", window, weight[first, second], preferred_element_type=F32
            )
    return total


def normalize(features, gain):
    scaled = (
        features
        * lax.rsqrt(jnp.mean(features * features, axis=-1, keepdims=True) + norm_eps)
        * gain
    )
    return jax.nn.silu(scaled).astype(BF)


def shards(
    queries,
    keys,
    values,
    keyboard,
    mouse,
    key_table,
    mouse_table,
    guidance,
    out_weight,
    latent,
    conv_in,
    gain,
    conv_out,
):
    rounds = lax.axis_size("x")
    sets = lax.axis_size("z")
    x = lax.axis_index("x")
    z = lax.axis_index("z")
    core = lax.axis_index("branch")
    rows = queries.shape[0]
    outs = out_weight.shape[1]
    frames = keyboard.shape[0]
    assert frames == rounds and rounds % 2 == 0

    packed = pack(core, queries, keys, values, out_weight, sets)
    own = lax.all_to_all(packed, "z", 0, 0, tiled=True)

    offsets = [0]
    for step in range(1, rounds // 2):
        offsets += [-step, step]
    offsets.append(rounds // 2)
    order = (x + jnp.array(offsets, dtype=jnp.int32)) % rounds
    bias, term = action_terms(
        core * sets + z, keyboard[order], mouse[order], key_table, mouse_table, out_weight
    )

    moving = own[:, rows:, :]
    results = [frame_attention(own, [own], rows, rows, outs)]
    low = high = moving
    for step in range(1, rounds // 2):
        low = lax.ppermute(low, "x", ring(rounds, 1))
        high = lax.ppermute(high, "x", ring(rounds, -1))
        results.append(frame_attention(own, [low], rows, 0, outs))
        results.append(frame_attention(own, [high], rows, 0, outs))
    cut = sets // 2
    low = lax.ppermute(low[:cut], "x", ring(rounds, 1))
    high = lax.ppermute(high[cut:], "x", ring(rounds, -1))
    results.append(frame_attention(own, [low, high], rows, 0, outs))
    sums, stats = zip(*results)
    part = guide(guidance, own, bias, term, sums, stats, rows, outs)
    returned = lax.all_to_all(part, "z", 0, 0, tiled=True)
    mine = jnp.sum(returned.astype(F32), axis=0)
    other = lax.ppermute(mine, "branch", [(0, 1), (1, 0)])
    both = mine + other
    velocity = jnp.concatenate([both[:, :outs], both[:, outs:]], axis=0)

    stepped = (latent - step_size * velocity).astype(BF)
    half = rows // 2
    flat = jnp.concatenate([stepped[:half], stepped[half:]], axis=1)
    count = rounds * sets
    index = x * sets + z
    forward = [(i, i + 1) for i in range(count - 1)]
    backward = [(i + 1, i) for i in range(count - 1)]
    before = lax.ppermute(flat, ("x", "z"), forward)
    after = lax.ppermute(flat, ("x", "z"), backward)

    def as_grid(block):
        block = jnp.concatenate([block[:, :outs], block[:, outs:]], axis=0)
        return block.reshape(rows, 2, 2, -1).transpose(1, 0, 2, 3).reshape(2, 2 * rows, -1)

    top_edge = index == 0
    bottom_edge = index == count - 1
    widened = jnp.concatenate([as_grid(before), as_grid(flat), as_grid(after)], axis=0)
    widened = clear_rows(widened, 2, top_edge, bottom_edge)
    hidden = normalize(convolve(widened, conv_in), gain)
    hidden = clear_rows(hidden, 1, top_edge, bottom_edge)
    colours = convolve(hidden, conv_out)
    return (velocity, colours.transpose(2, 0, 1))


def solution(mesh):
    cores = mesh.shape["branch"]
    tok = mesh.shape["tok"]

    def run(*arrays):
        sets = min(arrays[0].shape[1] // (HEAD_DIM * cores), tok)
        fine = Mesh(
            mesh.devices.reshape(mesh.shape["groups"], cores, tok // sets, sets),
            ("groups", "branch", "x", "z"),
        )
        tokens = P(("groups", "x", "z"), None)
        placed = (
            tokens,
            tokens,
            tokens,
            P("groups"),
            P("groups"),
            P(),
            P(),
            P(),
            P(),
            tokens,
            P(),
            P(),
            P(),
        )
        return jax.shard_map(
            shards,
            mesh=fine,
            in_specs=placed,
            out_specs=(tokens, P(None, ("groups", "x", "z"), None)),
            check_vma=False,
        )(*arrays)

    return run
```

```python
import functools
import math

import jax
import jax.numpy as jnp
from jax import lax
from jax.experimental import pallas as pl
from jax.experimental.pallas import tpu as pltpu
from jax.sharding import Mesh
from jax.sharding import PartitionSpec as P

HEAD_DIM = 128

step_size = 0.25
norm_eps = 1e-06
TO_EXP2 = HEAD_DIM ** (-0.5) / math.log(2.0)
BF = jnp.bfloat16
F32 = jnp.float32
VMEM = pl.BlockSpec(memory_space=pltpu.VMEM)
SMEM = pl.BlockSpec(memory_space=pltpu.SMEM)


def dot(a, b, dims, **kw):
    return lax.dot_general(a, b, (dims, ((), ())), preferred_element_type=F32, **kw)


def pack_kernel(core_ref, q_ref, k_ref, v_ref, w_ref, out_ref):
    sets, _, hd = out_ref.shape
    rows = q_ref.shape[0]
    half = rows // 2
    for z in range(sets):
        cols = slice(z * hd, (z + 1) * hd)
        out_ref[z, 0:rows, :] = q_ref[:, cols]
        out_ref[z, rows : 2 * rows, :] = k_ref[:, cols]
        projected = dot(v_ref[:, cols], w_ref[:, cols], ((1,), (1,))).astype(BF)
        out_ref[z, 2 * rows :, :] = jnp.concatenate([projected[:half], projected[half:]], axis=1)


def pack(core, queries, keys, values, weight_t, sets):
    rows = queries.shape[0]
    cols = sets * HEAD_DIM
    outs = weight_t.shape[0]
    block = pl.BlockSpec((rows, cols), lambda i, c: (0, c[0]))
    return pl.pallas_call(
        pack_kernel,
        grid_spec=pltpu.PrefetchScalarGridSpec(
            num_scalar_prefetch=1,
            grid=(1,),
            in_specs=[block, block, block, pl.BlockSpec((outs, cols), lambda i, c: (0, c[0]))],
            out_specs=VMEM,
        ),
        out_shape=jax.ShapeDtypeStruct((sets, 2 * rows + rows // 2, HEAD_DIM), BF),
        name="pack",
    )(core[None], queries, keys, values, weight_t)


def terms_kernel(offsets, kb_ref, ms_ref, x_ref, head_ref, key_ref, mouse_ref, w_ref, bias_ref, term_ref):
    frames = len(offsets)
    places = [lax.rem(x_ref[0] + (frames + offset), frames) for offset in offsets]
    rows_key = jnp.concatenate([key_ref[pl.ds(kb_ref[at], 1)] for at in places], axis=0)
    rows_mouse = jnp.concatenate([mouse_ref[pl.ds(ms_ref[at], 1)] for at in places], axis=0)
    rows_key = rows_key.astype(F32)
    rows_mouse = rows_mouse.astype(F32)
    bias_key, bias_mouse = rows_key[:, 0, :], rows_mouse[:, 0, :]
    bias = [bias_key + bias_mouse, bias_mouse, bias_key, jnp.zeros_like(bias_key)]
    bias_ref[...] = jnp.concatenate(bias, axis=0).astype(BF)
    terms = jnp.concatenate([rows_key[:, 1, :], rows_mouse[:, 1, :]], axis=0).astype(BF)
    term_ref[...] = dot(terms, w_ref[...], ((1,), (1,)))


def action_terms(offsets, x, head, keyboard, mouse, key_table, mouse_table, weight_t):
    frames = len(offsets)
    outs = weight_t.shape[0]
    return pl.pallas_call(
        functools.partial(terms_kernel, offsets),
        grid_spec=pltpu.PrefetchScalarGridSpec(
            num_scalar_prefetch=4,
            grid=(1,),
            in_specs=[
                pl.BlockSpec(key_table.shape[:2] + (HEAD_DIM,), lambda i, a, b, x, h: (0, 0, h[0])),
                pl.BlockSpec(mouse_table.shape[:2] + (HEAD_DIM,), lambda i, a, b, x, h: (0, 0, h[0])),
                pl.BlockSpec((outs, HEAD_DIM), lambda i, a, b, x, h: (0, h[0])),
            ],
            out_specs=[VMEM, VMEM],
        ),
        out_shape=[
            jax.ShapeDtypeStruct((4 * frames, HEAD_DIM), BF),
            jax.ShapeDtypeStruct((2 * frames, outs), F32),
        ],
        name="terms",
    )(keyboard, mouse, x[None], head[None], key_table, mouse_table, weight_t)


def frame_kernel(rows, at, own_ref, *refs):
    kv_refs, (sum_ref, stat_ref) = refs[:-2], refs[-2:]
    sets, _, hd = own_ref.shape
    half = rows // 2
    outs = sum_ref.shape[0]
    query = own_ref[:, 0:rows, :].reshape(sets * rows, hd)

    def gathered(first, last):
        parts = [r[:, first:last, :].reshape(-1, hd) for r in kv_refs]
        return parts[0] if len(parts) == 1 else jnp.concatenate(parts, axis=0)

    key_low = gathered(at, at + half)
    key_high = gathered(at + half, at + rows)
    both = gathered(at + rows, at + rows + half)
    score_low = dot(key_low, query, ((1,), (1,)))
    score_high = dot(key_high, query, ((1,), (1,)))
    top = jnp.maximum(
        jnp.max(score_low, axis=0, keepdims=True), jnp.max(score_high, axis=0, keepdims=True)
    )
    raised_low = jnp.exp2((score_low - top) * TO_EXP2)
    raised_high = jnp.exp2((score_high - top) * TO_EXP2)
    total = jnp.sum(raised_low, axis=0, keepdims=True) + jnp.sum(raised_high, axis=0, keepdims=True)
    summed = dot(both[:, :outs], raised_low.astype(BF), ((0,), (0,)))
    summed = summed + dot(both[:, outs:], raised_high.astype(BF), ((0,), (0,)))
    sum_ref[...] = summed
    stat_ref[0:1, :] = top
    stat_ref[1:2, :] = total


def frame_attention(own, pieces, rows, at, outs):
    tokens = own.shape[0] * rows
    flops = 2 * tokens * tokens * (HEAD_DIM + outs)
    return pl.pallas_call(
        functools.partial(frame_kernel, rows, at),
        in_specs=[VMEM] * (1 + len(pieces)),
        out_specs=[VMEM, VMEM],
        out_shape=[
            jax.ShapeDtypeStruct((outs, tokens), F32),
            jax.ShapeDtypeStruct((2, tokens), F32),
        ],
        cost_estimate=pl.CostEstimate(
            flops=flops, transcendentals=tokens * tokens, bytes_accessed=1 << 20
        ),
        name="frame",
    )(own, *pieces)


def guide_kernel(rows, count, guide_ref, own_ref, bias_ref, term_ref, *refs):
    sum_refs, stat_refs, out_ref = refs[:count], refs[count : 2 * count], refs[-1]
    sets, _, hd = own_ref.shape
    half = rows // 2
    query = own_ref[:, 0:rows, :].reshape(sets * rows, hd)
    shift = dot(bias_ref[...], query, ((1,), (1,)))
    tops = jnp.concatenate([r[0:1, :] for r in stat_refs], axis=0)
    totals = jnp.concatenate([r[1:2, :] for r in stat_refs], axis=0)
    parts = []
    for b in range(4):
        height = (tops + shift[b * count : (b + 1) * count]) * TO_EXP2
        factor = jnp.exp2(height - jnp.max(height, axis=0, keepdims=True))
        total = jnp.sum(factor * totals, axis=0, keepdims=True)
        parts.append(factor * (guide_ref[b] / total))
    mix = (parts[0] + parts[1]) + (parts[2] + parts[3])
    loads = jnp.concatenate(
        [(parts[0] + parts[2]) * totals, (parts[0] + parts[1]) * totals], axis=0
    )
    result = dot(term_ref[...], loads, ((0,), (0,)), precision=lax.Precision.HIGHEST)
    for j in range(count):
        result = result + mix[j : j + 1, :] * sum_refs[j][...]
    by_token = jnp.transpose(result).reshape(sets, rows, -1)
    out_ref[...] = jnp.concatenate([by_token[:, :half], by_token[:, half:]], axis=2).astype(BF)


def guide(guidance, own, bias, term, sums, stats, rows, outs):
    sets = own.shape[0]
    count = len(sums)
    return pl.pallas_call(
        functools.partial(guide_kernel, rows, count),
        in_specs=[SMEM] + [VMEM] * (3 + 2 * count),
        out_specs=VMEM,
        out_shape=jax.ShapeDtypeStruct((sets, rows // 2, 2 * outs), BF),
        name="guide",
    )(guidance, own, bias, term, *sums, *stats)


def decode_kernel(index_ref, before_ref, mine_ref, after_ref, conv_in_ref, gain_ref, conv_out_ref, out_ref):
    outs = before_ref.shape[1] // 2
    lat = outs // 4
    tokens = before_ref.shape[0] * 2
    left, right = [], []
    for ref in (before_ref, mine_ref, after_ref):
        both = ref[...].astype(F32)
        block = jnp.concatenate([both[:, :outs], both[:, outs:]], axis=0)
        edge = jnp.zeros_like(block[:1])
        earlier = jnp.concatenate([edge, block[:-1]], axis=0)
        later = jnp.concatenate([block[1:], edge], axis=0)
        for dy in range(2):
            at = 2 * lat * dy
            here = block[:, at : at + 2 * lat]
            left.append(jnp.concatenate([earlier[:, at + lat : at + 2 * lat], here], axis=1))
            right.append(jnp.concatenate([here, later[:, at : at + lat]], axis=1))
    height = 4 * tokens
    row = lax.broadcasted_iota(jnp.int32, (height, 1), 0) // tokens
    first, last = index_ref[0] == 0, index_ref[0] == index_ref[1] - 1
    keep = jnp.where((row == 0) & first | (row == 3) & last, 0.0, 1.0)
    taps = []
    for windows in (left, right):
        stack = jnp.concatenate(windows, axis=0).astype(BF)
        features = dot(stack[:height], conv_in_ref[0], ((1,), (0,)))
        for a in range(1, 3):
            part = stack[a * tokens : a * tokens + height]
            features = features + dot(part, conv_in_ref[a], ((1,), (0,)))
        power = jnp.mean(features * features, axis=1, keepdims=True)
        scaled = features * lax.rsqrt(power + norm_eps) * gain_ref[...]
        normed = scaled / (1.0 + jnp.exp(-scaled)) * keep
        taps.append(dot(conv_out_ref[...], normed.astype(BF), ((1,), (1,))))
    even, odd = taps
    step = even.shape[0] // 3
    lane = lax.broadcasted_iota(jnp.int32, (step, height), 1) % tokens
    before = jnp.where(lane == 0, 0.0, pltpu.roll(odd[:step], 1, 1))
    after = jnp.where(lane == tokens - 1, 0.0, pltpu.roll(even[2 * step :], height - 1, 1))
    columns = [
        before + even[step : 2 * step] + odd[2 * step :],
        even[:step] + odd[step : 2 * step] + after,
    ]
    source = lax.broadcasted_iota(jnp.int32, (height, height), 0)
    target = lax.broadcasted_iota(jnp.int32, (height, height), 1)
    colours = None
    for dx, column in enumerate(columns):
        moved = column[0:3]
        for a in range(1, 3):
            moved = moved + pltpu.roll(column[3 * a : 3 * a + 3], height - a * tokens, 1)
        chosen = jnp.where(target == 2 * source + dx, 1.0, 0.0)
        placed = dot(moved, chosen, ((1,), (0,)), precision=lax.Precision.HIGHEST)
        colours = placed if colours is None else colours + placed
    out_ref[:, 0, :] = colours[:, : 2 * tokens]
    out_ref[:, 1, :] = colours[:, 2 * tokens :]


def decode(index, before, mine, after, conv_in, gain, conv_out):
    tokens = before.shape[0] * 2
    return pl.pallas_call(
        decode_kernel,
        in_specs=[SMEM] + [VMEM] * 6,
        out_specs=VMEM,
        out_shape=jax.ShapeDtypeStruct((3, 2, 2 * tokens), F32),
        name="decode",
    )(index, before, mine, after, conv_in, gain, conv_out)


def shifted(value, axis, count, steps):
    return lax.ppermute(value, axis, [(i, (i + steps) % count) for i in range(count)])


def shards(
    queries,
    keys,
    values,
    keyboard,
    mouse,
    key_table,
    mouse_table,
    guidance,
    out_weight,
    latent,
    conv_in,
    gain,
    conv_out,
):
    rounds = lax.axis_size("x")
    sets = lax.axis_size("z")
    x = lax.axis_index("x")
    z = lax.axis_index("z")
    core = lax.axis_index("branch")
    rows = queries.shape[0]
    outs = out_weight.shape[1]
    frames = keyboard.shape[0]
    assert frames == rounds and rounds % 4 == 0
    weight_t = out_weight.T
    packed = pack(core, queries, keys, values, weight_t, sets)
    own = lax.all_to_all(packed, "z", 0, 0, tiled=True)

    near = rounds // 4
    cut = sets // 2
    moving = own[:, rows:, :]
    low, high, offsets = {}, {}, [0]
    for step in range(1, near + 1):
        low[step] = shifted(moving, "x", rounds, step)
        high[step] = shifted(moving, "x", rounds, -step)
        offsets += [-step, step]
    for step in range(near + 1, 2 * near):
        offsets += [-step, step]
    offsets.append(2 * near)
    bias, term = action_terms(
        tuple(offsets), x, core * sets + z, keyboard, mouse, key_table, mouse_table, weight_t
    )

    def attention(*pieces):
        return frame_attention(own, pieces, rows, 0, outs)

    results = [frame_attention(own, [own], rows, rows, outs)]
    for step in range(1, near):
        results += [attention(low[step]), attention(high[step])]
    far_low, far_high, results, bias, term = lax.optimization_barrier(
        (low[near], high[near], results, bias, term)
    )
    for step in range(near + 1, 2 * near):
        low[step] = shifted(far_low, "x", rounds, step - near)
        high[step] = shifted(far_high, "x", rounds, near - step)
    half_low = shifted(far_low[:cut], "x", rounds, near)
    half_high = shifted(far_high[cut:], "x", rounds, -near)
    results += [attention(far_low), attention(far_high)]
    for step in range(near + 1, 2 * near):
        results += [attention(low[step]), attention(high[step])]
    results.append(attention(half_low, half_high))
    sums, stats = zip(*results)
    part = guide(guidance, own, bias, term, sums, stats, rows, outs)
    returned = lax.all_to_all(part, "z", 0, 0, tiled=True)
    mine = jnp.sum(returned.astype(F32), axis=0)
    other = lax.ppermute(mine, "branch", [(0, 1), (1, 0)])
    both = mine + other
    velocity = jnp.concatenate([both[:, :outs], both[:, outs:]], axis=0)

    half = rows // 2
    noisy = jnp.concatenate([latent[:half], latent[half:]], axis=1)
    stepped = (noisy - step_size * both).astype(BF)
    count = rounds * sets
    index = jnp.stack([x * sets + z, jnp.int32(count)])
    before = lax.ppermute(stepped, ("x", "z"), [(i, i + 1) for i in range(count - 1)])
    after = lax.ppermute(stepped, ("x", "z"), [(i + 1, i) for i in range(count - 1)])
    taps_in = conv_in.reshape(conv_in.shape[0], -1, conv_in.shape[3])
    taps_out = conv_out.transpose(1, 0, 3, 2).reshape(3, -1, conv_out.shape[2])
    taps_out = jnp.pad(taps_out, ((0, 0), (0, 16 - taps_out.shape[1]), (0, 0)))
    taps_out = taps_out.reshape(-1, conv_out.shape[2])
    colours = decode(index, before, stepped, after, taps_in, gain[None], taps_out)
    return (velocity, colours)


def solution(mesh):
    cores = mesh.shape["branch"]
    tok = mesh.shape["tok"]

    def run(*arrays):
        sets = min(arrays[0].shape[1] // (HEAD_DIM * cores), tok)
        fine = Mesh(
            mesh.devices.reshape(mesh.shape["groups"], cores, tok // sets, sets),
            ("groups", "branch", "x", "z"),
        )
        tokens = P(("groups", "x", "z"), None)
        placed = (
            tokens,
            tokens,
            tokens,
            P("groups"),
            P("groups"),
            P(),
            P(),
            P(),
            P(),
            tokens,
            P(),
            P(),
            P(),
        )
        return jax.shard_map(
            shards,
            mesh=fine,
            in_specs=placed,
            out_specs=(tokens, P(None, ("groups", "x", "z"), None)),
            check_vma=False,
        )(*arrays)

    return run
```

```python
import functools
import math

import jax
import jax.numpy as jnp
from jax import lax
from jax.experimental import pallas as pl
from jax.experimental.pallas import tpu as pltpu
from jax.sharding import Mesh
from jax.sharding import PartitionSpec as P

HEAD_DIM = 128

step_size = 0.25
norm_eps = 1e-06
TO_EXP2 = HEAD_DIM ** (-0.5) / math.log(2.0)
BF = jnp.bfloat16
F32 = jnp.float32
VMEM = pl.BlockSpec(memory_space=pltpu.VMEM)
SMEM = pl.BlockSpec(memory_space=pltpu.SMEM)
GRANT = pltpu.CompilerParams(vmem_limit_bytes=12 << 20)


def in_hbm(array):
    return pltpu.with_memory_space_constraint(array, pltpu.HBM)


def dot(a, b, dims, **kw):
    return lax.dot_general(a, b, (dims, ((), ())), preferred_element_type=F32, **kw)


def pack_kernel(core_ref, q_ref, k_ref, v_ref, w_ref, out_ref, v_tmp, w_tmp, sems):
    sets, _, hd = out_ref.shape
    rows = q_ref.shape[0]
    half = rows // 2
    first = pl.multiple_of(core_ref[0] * (sets * hd), hd)
    mine = pl.ds(first, sets * hd)
    copies = [
        pltpu.make_async_copy(w_ref.at[:, mine], w_tmp, sems.at[0]),
        pltpu.make_async_copy(v_ref.at[:, mine], v_tmp, sems.at[1]),
    ]
    for n, source in enumerate((q_ref, k_ref)):
        for z in range(sets):
            copies.append(
                pltpu.make_async_copy(
                    source.at[:, pl.ds(pl.multiple_of(first + z * hd, hd), hd)],
                    out_ref.at[z, pl.ds(n * rows, rows), :],
                    sems.at[len(copies)],
                )
            )
    for copy in copies:
        copy.start()
    for copy in copies[:2]:
        copy.wait()
    for z in range(sets):
        cols = slice(z * hd, (z + 1) * hd)
        projected = dot(v_tmp[:, cols], w_tmp[:, cols], ((1,), (1,))).astype(BF)
        out_ref[z, 2 * rows :, :] = jnp.concatenate([projected[:half], projected[half:]], axis=1)
    for copy in copies[2:]:
        copy.wait()


def pack(core, queries, keys, values, weight_t, sets):
    rows = queries.shape[0]
    cols = sets * HEAD_DIM
    hbm = pl.BlockSpec(memory_space=pltpu.HBM)
    return pl.pallas_call(
        pack_kernel,
        in_specs=[SMEM, hbm, hbm, hbm, hbm],
        out_specs=VMEM,
        out_shape=jax.ShapeDtypeStruct((sets, 2 * rows + rows // 2, HEAD_DIM), BF),
        scratch_shapes=[
            pltpu.VMEM((rows, cols), BF),
            pltpu.VMEM((weight_t.shape[0], cols), BF),
            pltpu.SemaphoreType.DMA((2 + 2 * sets,)),
        ],
        name="pack",
        compiler_params=GRANT,
    )(core[None], *(in_hbm(a) for a in (queries, keys, values, weight_t)))


def terms_kernel(offsets, kb_ref, ms_ref, x_ref, head_ref, key_ref, mouse_ref, w_ref, bias_ref, term_ref):
    frames = len(offsets)
    places = [lax.rem(x_ref[0] + (frames + offset), frames) for offset in offsets]
    rows_key = jnp.concatenate([key_ref[pl.ds(kb_ref[at], 1)] for at in places], axis=0)
    rows_mouse = jnp.concatenate([mouse_ref[pl.ds(ms_ref[at], 1)] for at in places], axis=0)
    rows_key = rows_key.astype(F32)
    rows_mouse = rows_mouse.astype(F32)
    bias_key, bias_mouse = rows_key[:, 0, :], rows_mouse[:, 0, :]
    bias = [bias_key + bias_mouse, bias_mouse, bias_key, jnp.zeros_like(bias_key)]
    bias_ref[...] = jnp.concatenate(bias, axis=0).astype(BF)
    terms = jnp.concatenate([rows_key[:, 1, :], rows_mouse[:, 1, :]], axis=0).astype(BF)
    term_ref[...] = dot(terms, w_ref[...], ((1,), (1,)))


def action_terms(offsets, x, head, keyboard, mouse, key_table, mouse_table, weight_t):
    frames = len(offsets)
    outs = weight_t.shape[0]
    return pl.pallas_call(
        functools.partial(terms_kernel, offsets),
        grid_spec=pltpu.PrefetchScalarGridSpec(
            num_scalar_prefetch=4,
            grid=(1,),
            in_specs=[
                pl.BlockSpec(key_table.shape[:2] + (HEAD_DIM,), lambda i, a, b, x, h: (0, 0, h[0])),
                pl.BlockSpec(mouse_table.shape[:2] + (HEAD_DIM,), lambda i, a, b, x, h: (0, 0, h[0])),
                pl.BlockSpec((outs, HEAD_DIM), lambda i, a, b, x, h: (0, h[0])),
            ],
            out_specs=[VMEM, VMEM],
        ),
        out_shape=[
            jax.ShapeDtypeStruct((4 * frames, HEAD_DIM), BF),
            jax.ShapeDtypeStruct((2 * frames, outs), F32),
        ],
        name="terms",
        compiler_params=GRANT,
    )(keyboard, mouse, x[None], head[None], key_table, mouse_table, weight_t)


def frame_kernel(rows, at, own_ref, *refs):
    kv_refs, (sum_ref, stat_ref) = refs[:-2], refs[-2:]
    sets, _, hd = own_ref.shape
    half = rows // 2
    outs = sum_ref.shape[0]
    query = own_ref[:, 0:rows, :].reshape(sets * rows, hd)

    def gathered(first, last):
        parts = [r[:, first:last, :].reshape(-1, hd) for r in kv_refs]
        return parts[0] if len(parts) == 1 else jnp.concatenate(parts, axis=0)

    key_low = gathered(at, at + half)
    key_high = gathered(at + half, at + rows)
    both = gathered(at + rows, at + rows + half)
    score_low = dot(key_low, query, ((1,), (1,)))
    score_high = dot(key_high, query, ((1,), (1,)))
    top = jnp.maximum(
        jnp.max(score_low, axis=0, keepdims=True), jnp.max(score_high, axis=0, keepdims=True)
    )
    raised_low = jnp.exp2((score_low - top) * TO_EXP2)
    raised_high = jnp.exp2((score_high - top) * TO_EXP2)
    total = jnp.sum(raised_low, axis=0, keepdims=True) + jnp.sum(raised_high, axis=0, keepdims=True)
    summed = dot(both[:, :outs], raised_low.astype(BF), ((0,), (0,)))
    summed = summed + dot(both[:, outs:], raised_high.astype(BF), ((0,), (0,)))
    sum_ref[...] = summed
    stat_ref[0:1, :] = top
    stat_ref[1:2, :] = total


def frame_attention(own, pieces, rows, at, outs):
    tokens = own.shape[0] * rows
    flops = 2 * tokens * tokens * (HEAD_DIM + outs)
    return pl.pallas_call(
        functools.partial(frame_kernel, rows, at),
        in_specs=[VMEM] * (1 + len(pieces)),
        out_specs=[VMEM, VMEM],
        out_shape=[
            jax.ShapeDtypeStruct((outs, tokens), F32),
            jax.ShapeDtypeStruct((2, tokens), F32),
        ],
        cost_estimate=pl.CostEstimate(
            flops=flops, transcendentals=tokens * tokens, bytes_accessed=1 << 20
        ),
        name="frame",
        compiler_params=GRANT,
    )(own, *pieces)


def guide_kernel(rows, count, guide_ref, own_ref, bias_ref, term_ref, *refs):
    sum_refs, stat_refs, out_ref = refs[:count], refs[count : 2 * count], refs[-1]
    sets, _, hd = own_ref.shape
    half = rows // 2
    query = own_ref[:, 0:rows, :].reshape(sets * rows, hd)
    shift = dot(bias_ref[...], query, ((1,), (1,)))
    tops = jnp.concatenate([r[0:1, :] for r in stat_refs], axis=0)
    totals = jnp.concatenate([r[1:2, :] for r in stat_refs], axis=0)
    parts = []
    for b in range(4):
        height = (tops + shift[b * count : (b + 1) * count]) * TO_EXP2
        factor = jnp.exp2(height - jnp.max(height, axis=0, keepdims=True))
        total = jnp.sum(factor * totals, axis=0, keepdims=True)
        parts.append(factor * (guide_ref[b] / total))
    mix = (parts[0] + parts[1]) + (parts[2] + parts[3])
    loads = jnp.concatenate(
        [(parts[0] + parts[2]) * totals, (parts[0] + parts[1]) * totals], axis=0
    )
    result = dot(term_ref[...], loads, ((0,), (0,)), precision=lax.Precision.HIGHEST)
    for j in range(count):
        result = result + mix[j : j + 1, :] * sum_refs[j][...]
    by_token = jnp.transpose(result).reshape(sets, rows, -1)
    out_ref[...] = jnp.concatenate([by_token[:, :half], by_token[:, half:]], axis=2).astype(BF)


def guide(guidance, own, bias, term, sums, stats, rows, outs):
    sets = own.shape[0]
    count = len(sums)
    return pl.pallas_call(
        functools.partial(guide_kernel, rows, count),
        in_specs=[SMEM] + [VMEM] * (3 + 2 * count),
        out_specs=VMEM,
        out_shape=jax.ShapeDtypeStruct((sets, rows // 2, 2 * outs), BF),
        name="guide",
        compiler_params=GRANT,
    )(guidance, own, bias, term, *sums, *stats)


def decode_kernel(index_ref, before_ref, mine_ref, after_ref, conv_in_ref, gain_ref, conv_out_ref, out_ref):
    outs = before_ref.shape[1] // 2
    lat = outs // 4
    tokens = before_ref.shape[0] * 2
    left, right = [], []
    for ref in (before_ref, mine_ref, after_ref):
        both = ref[...].astype(F32)
        block = jnp.concatenate([both[:, :outs], both[:, outs:]], axis=0)
        edge = jnp.zeros_like(block[:1])
        earlier = jnp.concatenate([edge, block[:-1]], axis=0)
        later = jnp.concatenate([block[1:], edge], axis=0)
        for dy in range(2):
            at = 2 * lat * dy
            here = block[:, at : at + 2 * lat]
            left.append(jnp.concatenate([earlier[:, at + lat : at + 2 * lat], here], axis=1))
            right.append(jnp.concatenate([here, later[:, at : at + lat]], axis=1))
    height = 4 * tokens
    row = lax.broadcasted_iota(jnp.int32, (height, 1), 0) // tokens
    first, last = index_ref[0] == 0, index_ref[0] == index_ref[1] - 1
    keep = jnp.where((row == 0) & first | (row == 3) & last, 0.0, 1.0)
    taps = []
    for windows in (left, right):
        stack = jnp.concatenate(windows, axis=0).astype(BF)
        features = dot(stack[:height], conv_in_ref[0], ((1,), (0,)))
        for a in range(1, 3):
            part = stack[a * tokens : a * tokens + height]
            features = features + dot(part, conv_in_ref[a], ((1,), (0,)))
        power = jnp.mean(features * features, axis=1, keepdims=True)
        scaled = features * lax.rsqrt(power + norm_eps) * gain_ref[...]
        normed = scaled / (1.0 + jnp.exp(-scaled)) * keep
        taps.append(dot(conv_out_ref[...], normed.astype(BF), ((1,), (1,))))
    even, odd = taps
    step = even.shape[0] // 3
    lane = lax.broadcasted_iota(jnp.int32, (step, height), 1) % tokens
    before = jnp.where(lane == 0, 0.0, pltpu.roll(odd[:step], 1, 1))
    after = jnp.where(lane == tokens - 1, 0.0, pltpu.roll(even[2 * step :], height - 1, 1))
    columns = [
        before + even[step : 2 * step] + odd[2 * step :],
        even[:step] + odd[step : 2 * step] + after,
    ]
    source = lax.broadcasted_iota(jnp.int32, (height, height), 0)
    target = lax.broadcasted_iota(jnp.int32, (height, height), 1)
    colours = None
    for dx, column in enumerate(columns):
        moved = column[0:3]
        for a in range(1, 3):
            moved = moved + pltpu.roll(column[3 * a : 3 * a + 3], height - a * tokens, 1)
        chosen = jnp.where(target == 2 * source + dx, 1.0, 0.0)
        placed = dot(moved, chosen, ((1,), (0,)), precision=lax.Precision.HIGHEST)
        colours = placed if colours is None else colours + placed
    out_ref[:, 0, :] = colours[:, : 2 * tokens]
    out_ref[:, 1, :] = colours[:, 2 * tokens :]


def decode(index, before, mine, after, conv_in, gain, conv_out):
    tokens = before.shape[0] * 2
    return pl.pallas_call(
        decode_kernel,
        in_specs=[SMEM] + [VMEM] * 6,
        out_specs=VMEM,
        out_shape=jax.ShapeDtypeStruct((3, 2, 2 * tokens), F32),
        name="decode",
        compiler_params=GRANT,
    )(index, before, mine, after, conv_in, gain, conv_out)


def shifted(value, axis, count, steps):
    return lax.ppermute(value, axis, [(i, (i + steps) % count) for i in range(count)])


def shards(
    queries,
    keys,
    values,
    keyboard,
    mouse,
    key_table,
    mouse_table,
    guidance,
    out_weight,
    latent,
    conv_in,
    gain,
    conv_out,
):
    rounds = lax.axis_size("x")
    sets = lax.axis_size("z")
    x = lax.axis_index("x")
    z = lax.axis_index("z")
    core = lax.axis_index("branch")
    rows = queries.shape[0]
    outs = out_weight.shape[1]
    frames = keyboard.shape[0]
    assert frames == rounds and rounds % 4 == 0
    weight_t = out_weight.T
    packed = pack(core, queries, keys, values, weight_t, sets)
    own = lax.all_to_all(packed, "z", 0, 0, tiled=True)

    near = rounds // 4
    cut = sets // 2
    moving = own[:, rows:, :]
    low, high, offsets = {}, {}, [0]
    for step in range(1, near + 1):
        low[step] = shifted(moving, "x", rounds, step)
        high[step] = shifted(moving, "x", rounds, -step)
        offsets += [-step, step]
    for step in range(near + 1, 2 * near):
        offsets += [-step, step]
    offsets.append(2 * near)
    bias, term = action_terms(
        tuple(offsets), x, core * sets + z, keyboard, mouse, key_table, mouse_table, weight_t
    )

    def attention(*pieces):
        return frame_attention(own, pieces, rows, 0, outs)

    results = [frame_attention(own, [own], rows, rows, outs)]
    for step in range(1, near):
        results += [attention(low[step]), attention(high[step])]
    far_low, far_high, results, bias, term = lax.optimization_barrier(
        (low[near], high[near], results, bias, term)
    )
    for step in range(near + 1, 2 * near):
        low[step] = shifted(far_low, "x", rounds, step - near)
        high[step] = shifted(far_high, "x", rounds, near - step)
    half_low = shifted(far_low[:cut], "x", rounds, near)
    half_high = shifted(far_high[cut:], "x", rounds, -near)
    results += [attention(far_low), attention(far_high)]
    for step in range(near + 1, 2 * near):
        results += [attention(low[step]), attention(high[step])]
    results.append(attention(half_low, half_high))
    sums, stats = zip(*results)
    part = guide(guidance, own, bias, term, sums, stats, rows, outs)
    returned = lax.all_to_all(part, "z", 0, 0, tiled=True)
    mine = jnp.sum(returned.astype(F32), axis=0)
    other = lax.ppermute(mine, "branch", [(0, 1), (1, 0)])
    both = mine + other
    velocity = jnp.concatenate([both[:, :outs], both[:, outs:]], axis=0)

    half = rows // 2
    noisy = jnp.concatenate([latent[:half], latent[half:]], axis=1)
    stepped = (noisy - step_size * both).astype(BF)
    count = rounds * sets
    index = jnp.stack([x * sets + z, jnp.int32(count)])
    before = lax.ppermute(stepped, ("x", "z"), [(i, i + 1) for i in range(count - 1)])
    after = lax.ppermute(stepped, ("x", "z"), [(i + 1, i) for i in range(count - 1)])
    taps_in = conv_in.reshape(conv_in.shape[0], -1, conv_in.shape[3])
    taps_out = conv_out.transpose(1, 0, 3, 2).reshape(3, -1, conv_out.shape[2])
    taps_out = jnp.pad(taps_out, ((0, 0), (0, 16 - taps_out.shape[1]), (0, 0)))
    taps_out = taps_out.reshape(-1, conv_out.shape[2])
    colours = decode(index, before, stepped, after, taps_in, gain[None], taps_out)
    return (velocity, colours)


def solution(mesh):
    cores = mesh.shape["branch"]
    tok = mesh.shape["tok"]

    def run(*arrays):
        sets = min(arrays[0].shape[1] // (HEAD_DIM * cores), tok)
        fine = Mesh(
            mesh.devices.reshape(mesh.shape["groups"], cores, tok // sets, sets),
            ("groups", "branch", "x", "z"),
        )
        tokens = P(("groups", "x", "z"), None)
        placed = (
            tokens,
            tokens,
            tokens,
            P("groups"),
            P("groups"),
            P(),
            P(),
            P(),
            P(),
            tokens,
            P(),
            P(),
            P(),
        )
        return jax.shard_map(
            shards,
            mesh=fine,
            in_specs=placed,
            out_specs=(tokens, P(None, ("groups", "x", "z"), None)),
            check_vma=False,
        )(*arrays)

    return run
```

```python
import functools
import math

import jax
import jax.numpy as jnp
from jax import lax
from jax.experimental import pallas as pl
from jax.experimental.pallas import tpu as pltpu
from jax.sharding import Mesh
from jax.sharding import PartitionSpec as P

HEAD_DIM = 128

step_size = 0.25
norm_eps = 1e-06
TO_EXP2 = HEAD_DIM ** (-0.5) / math.log(2.0)
BF = jnp.bfloat16
F32 = jnp.float32
VMEM = pl.BlockSpec(memory_space=pltpu.VMEM)
SMEM = pl.BlockSpec(memory_space=pltpu.SMEM)
GRANT = pltpu.CompilerParams(vmem_limit_bytes=12 << 20)


def in_hbm(array):
    return pltpu.with_memory_space_constraint(array, pltpu.HBM)


def dot(a, b, dims, **kw):
    return lax.dot_general(a, b, (dims, ((), ())), preferred_element_type=F32, **kw)


def pack_kernel(core_ref, q_ref, k_ref, v_ref, w_ref, out_ref, q_tmp, k_tmp, v_tmp, w_tmp, sems):
    heads, _, hd = out_ref.shape
    rows = q_tmp.shape[0]
    half = rows // 2
    mine = pl.ds(pl.multiple_of(core_ref[0] * rows, rows), rows)
    copies = [
        pltpu.make_async_copy(w_ref, w_tmp, sems.at[0]),
        pltpu.make_async_copy(v_ref.at[mine, :], v_tmp, sems.at[1]),
        pltpu.make_async_copy(q_ref.at[mine, :], q_tmp, sems.at[2]),
        pltpu.make_async_copy(k_ref.at[mine, :], k_tmp, sems.at[3]),
    ]
    for copy in copies:
        copy.start()
    for copy in copies:
        copy.wait()
    for h in range(heads):
        cols = slice(h * hd, (h + 1) * hd)
        out_ref[h, 0:rows, :] = q_tmp[:, cols]
        out_ref[h, rows : 2 * rows, :] = k_tmp[:, cols]
        projected = dot(v_tmp[:, cols], w_tmp[:, cols], ((1,), (1,)))
        projected = jnp.concatenate([projected[:half], projected[half:]], axis=1)
        out_ref[h, 2 * rows :, :] = projected.astype(BF)


def pack(core, queries, keys, values, weight_t, rows):
    width = queries.shape[1]
    heads = width // HEAD_DIM
    hbm = pl.BlockSpec(memory_space=pltpu.HBM)
    return pl.pallas_call(
        pack_kernel,
        in_specs=[SMEM, hbm, hbm, hbm, hbm],
        out_specs=VMEM,
        out_shape=jax.ShapeDtypeStruct((heads, 2 * rows + rows // 2, HEAD_DIM), BF),
        scratch_shapes=[pltpu.VMEM((rows, width), BF)] * 3
        + [pltpu.VMEM(weight_t.shape, BF), pltpu.SemaphoreType.DMA((4,))],
        name="pack",
        compiler_params=GRANT,
    )(core[None], *(in_hbm(a) for a in (queries, keys, values, weight_t)))


def terms_kernel(order, kb_ref, ms_ref, head_ref, key_ref, mouse_ref, w_ref, bias_ref, term_ref):
    rows_key = jnp.concatenate([key_ref[pl.ds(kb_ref[f], 1)] for f in order], axis=0)
    rows_mouse = jnp.concatenate([mouse_ref[pl.ds(ms_ref[f], 1)] for f in order], axis=0)
    rows_key = rows_key.astype(F32)
    rows_mouse = rows_mouse.astype(F32)
    bias_key, bias_mouse = rows_key[:, 0, :], rows_mouse[:, 0, :]
    bias = [bias_key + bias_mouse, bias_mouse, bias_key, jnp.zeros_like(bias_key)]
    bias_ref[...] = jnp.concatenate(bias, axis=0).astype(BF)
    terms = jnp.concatenate([rows_key[:, 1, :], rows_mouse[:, 1, :]], axis=0).astype(BF)
    term_ref[...] = dot(terms, w_ref[...], ((1,), (1,)))


def action_terms(order, head, keyboard, mouse, key_table, mouse_table, weight_t):
    frames = len(order)
    outs = weight_t.shape[0]
    return pl.pallas_call(
        functools.partial(terms_kernel, order),
        grid_spec=pltpu.PrefetchScalarGridSpec(
            num_scalar_prefetch=3,
            grid=(1,),
            in_specs=[
                pl.BlockSpec(key_table.shape[:2] + (HEAD_DIM,), lambda i, a, b, h: (0, 0, h[0])),
                pl.BlockSpec(mouse_table.shape[:2] + (HEAD_DIM,), lambda i, a, b, h: (0, 0, h[0])),
                pl.BlockSpec((outs, HEAD_DIM), lambda i, a, b, h: (0, h[0])),
            ],
            out_specs=[VMEM, VMEM],
        ),
        out_shape=[
            jax.ShapeDtypeStruct((4 * frames, HEAD_DIM), BF),
            jax.ShapeDtypeStruct((2 * frames, outs), F32),
        ],
        name="terms",
        compiler_params=GRANT,
    )(keyboard, mouse, head[None], key_table, mouse_table, weight_t)


def share_kernel(rows, sets, own_ref, share_ref, sum_ref, top_ref, total_ref):
    heads, _, hd = own_ref.shape
    half = rows // 2
    outs = sum_ref.shape[1]
    query = own_ref[:, 0:rows, :].reshape(heads * rows, hd)
    gathered, per_gather = share_ref.shape[0], heads // sets
    for at in range(gathered):
        for part in range(per_gather):
            frame = at * per_gather + part
            place = slice(part * sets, (part + 1) * sets)
            keys = share_ref[at, place, 0:rows, :].reshape(sets * rows, hd)
            values = share_ref[at, place, rows:, :].reshape(sets * half, hd)
            scores = dot(keys, query, ((1,), (1,)))
            top = jnp.max(scores, axis=0, keepdims=True)
            raised = jnp.exp2((scores - top) * TO_EXP2)
            top_ref[frame : frame + 1, :] = top
            total_ref[frame : frame + 1, :] = jnp.sum(raised, axis=0, keepdims=True)
            raised = raised.reshape(sets, 2, half, -1)
            low = raised[:, 0].reshape(sets * half, -1).astype(BF)
            high = raised[:, 1].reshape(sets * half, -1).astype(BF)
            summed = dot(values[:, :outs], low, ((0,), (0,)))
            sum_ref[frame] = summed + dot(values[:, outs:], high, ((0,), (0,)))


def share_attention(own, share, rows, sets, outs):
    heads = own.shape[0]
    tokens = heads * rows
    frames = share.shape[0] * heads // sets
    keys = frames * sets * rows
    return pl.pallas_call(
        functools.partial(share_kernel, rows, sets),
        in_specs=[VMEM, VMEM],
        out_specs=[VMEM, VMEM, VMEM],
        out_shape=[
            jax.ShapeDtypeStruct((frames, outs, tokens), F32),
            jax.ShapeDtypeStruct((frames, tokens), F32),
            jax.ShapeDtypeStruct((frames, tokens), F32),
        ],
        cost_estimate=pl.CostEstimate(
            flops=2 * tokens * keys * (HEAD_DIM + outs),
            transcendentals=tokens * keys,
            bytes_accessed=1 << 20,
        ),
        name="share",
        compiler_params=GRANT,
    )(own, share)


def guide_kernel(rows, guide_ref, own_ref, bias_ref, term_ref, *refs):
    shares, out_ref = refs[:-1], refs[-1]
    sum_refs, top_refs, total_refs = shares[0::3], shares[1::3], shares[2::3]
    heads, _, hd = own_ref.shape
    half = rows // 2
    count = top_refs[0].shape[0]
    query = own_ref[:, 0:rows, :].reshape(heads * rows, hd)
    shift = dot(bias_ref[...], query, ((1,), (1,)))
    tops = [r[...] for r in top_refs]
    totals = [r[...] for r in total_refs]
    mixes = [None] * len(tops)
    by_key, by_mouse = None, None
    for b in range(4):
        heights = [(top + shift[b * count : (b + 1) * count]) * TO_EXP2 for top in tops]
        peak = functools.reduce(jnp.maximum, heights)
        peak = jnp.max(peak, axis=0, keepdims=True)
        factors = [jnp.exp2(height - peak) for height in heights]
        loads = functools.reduce(jnp.add, [f * t for f, t in zip(factors, totals)])
        scale = guide_ref[b] / jnp.sum(loads, axis=0, keepdims=True)
        parts = [f * scale for f in factors]
        mixes = [p if m is None else m + p for m, p in zip(mixes, parts)]
        loads = loads * scale
        if b % 2 == 0:
            by_key = loads if by_key is None else by_key + loads
        if b < 2:
            by_mouse = loads if by_mouse is None else by_mouse + loads
    loads = jnp.concatenate([by_key, by_mouse], axis=0)
    result = dot(term_ref[...], loads, ((0,), (0,)), precision=lax.Precision.HIGHEST)
    for mix, sum_ref in zip(mixes, sum_refs):
        for frame in range(count):
            result = result + mix[frame : frame + 1, :] * sum_ref[frame]
    by_token = jnp.transpose(result).reshape(heads, 2, half, -1)
    packed = jnp.concatenate([by_token[:, 0], by_token[:, 1]], axis=2)
    out_ref[...] = packed.astype(BF)


def guide(guidance, own, bias, term, shares, rows, outs):
    heads = own.shape[0]
    arrays = [array for share in shares for array in share]
    return pl.pallas_call(
        functools.partial(guide_kernel, rows),
        in_specs=[SMEM] + [VMEM] * (3 + len(arrays)),
        out_specs=VMEM,
        out_shape=jax.ShapeDtypeStruct((heads, rows // 2, 2 * outs), BF),
        name="guide",
        compiler_params=GRANT,
    )(guidance, own, bias, term, *arrays)


def decode_kernel(index_ref, before_ref, mine_ref, after_ref, conv_in_ref, gain_ref, conv_out_ref, out_ref):
    outs = before_ref.shape[1] // 2
    lat = outs // 4
    tokens = before_ref.shape[0] * 2
    left, right = [], []
    for ref in (before_ref, mine_ref, after_ref):
        both = ref[...].astype(F32)
        quarter = tokens // 4
        parts = [both[:quarter], both[quarter:]]
        parts = [p[:, side] for p in parts for side in (slice(0, outs), slice(outs, None))]
        block = jnp.concatenate(parts, axis=0)
        edge = jnp.zeros_like(block[:1])
        earlier = jnp.concatenate([edge, block[:-1]], axis=0)
        later = jnp.concatenate([block[1:], edge], axis=0)
        for dy in range(2):
            at = 2 * lat * dy
            here = block[:, at : at + 2 * lat]
            left.append(jnp.concatenate([earlier[:, at + lat : at + 2 * lat], here], axis=1))
            right.append(jnp.concatenate([here, later[:, at : at + lat]], axis=1))
    height = 4 * tokens
    row = lax.broadcasted_iota(jnp.int32, (height, 1), 0) // tokens
    first, last = index_ref[0] == 0, index_ref[0] == index_ref[1] - 1
    keep = jnp.where((row == 0) & first | (row == 3) & last, 0.0, 1.0)
    taps = []
    for windows in (left, right):
        stack = jnp.concatenate(windows, axis=0).astype(BF)
        features = dot(stack[:height], conv_in_ref[0], ((1,), (0,)))
        for a in range(1, 3):
            part = stack[a * tokens : a * tokens + height]
            features = features + dot(part, conv_in_ref[a], ((1,), (0,)))
        power = jnp.mean(features * features, axis=1, keepdims=True)
        scaled = features * lax.rsqrt(power + norm_eps) * gain_ref[...]
        normed = scaled / (1.0 + jnp.exp(-scaled)) * keep
        taps.append(dot(conv_out_ref[...], normed.astype(BF), ((1,), (1,))))
    even, odd = taps
    step = even.shape[0] // 3
    lane = lax.broadcasted_iota(jnp.int32, (step, height), 1) % tokens
    before = jnp.where(lane == 0, 0.0, pltpu.roll(odd[:step], 1, 1))
    after = jnp.where(lane == tokens - 1, 0.0, pltpu.roll(even[2 * step :], height - 1, 1))
    columns = [
        before + even[step : 2 * step] + odd[2 * step :],
        even[:step] + odd[step : 2 * step] + after,
    ]
    source = lax.broadcasted_iota(jnp.int32, (height, height), 0)
    target = lax.broadcasted_iota(jnp.int32, (height, height), 1)
    colours = None
    for dx, column in enumerate(columns):
        moved = column[0:3]
        for a in range(1, 3):
            moved = moved + pltpu.roll(column[3 * a : 3 * a + 3], height - a * tokens, 1)
        chosen = jnp.where(target == 2 * source + dx, 1.0, 0.0)
        placed = dot(moved, chosen, ((1,), (0,)), precision=lax.Precision.HIGHEST)
        colours = placed if colours is None else colours + placed
    out_ref[:, 0, :] = colours[:, : 2 * tokens]
    out_ref[:, 1, :] = colours[:, 2 * tokens :]


def decode(index, before, mine, after, conv_in, gain, conv_out):
    tokens = before.shape[0] * 2
    return pl.pallas_call(
        decode_kernel,
        in_specs=[SMEM] + [VMEM] * 6,
        out_specs=VMEM,
        out_shape=jax.ShapeDtypeStruct((3, 2, 2 * tokens), F32),
        name="decode",
        compiler_params=GRANT,
    )(index, before, mine, after, conv_in, gain, conv_out)


def shards(
    queries,
    keys,
    values,
    keyboard,
    mouse,
    key_table,
    mouse_table,
    guidance,
    out_weight,
    latent,
    conv_in,
    gain,
    conv_out,
):
    wide, narrow, sets = lax.axis_size("xh"), lax.axis_size("xl"), lax.axis_size("z")
    xh, xl, z = lax.axis_index("xh"), lax.axis_index("xl"), lax.axis_index("z")
    cores = lax.axis_size("branch")
    core = lax.axis_index("branch")
    outs = out_weight.shape[1]
    frames = keyboard.shape[0]
    assert frames == wide * narrow and cores == 2
    rows = queries.shape[0] // cores
    swap = [(0, 1), (1, 0)]

    weight_t = out_weight.T
    packed = pack(core, queries, keys, values, weight_t, rows)
    own = lax.all_to_all(packed, ("xh", "z"), 0, 0, tiled=True)
    share = lax.all_gather(own[:, rows:, :], "xl")
    other_share = lax.ppermute(share, "branch", swap)
    order = tuple(part * narrow + at for at in range(narrow) for part in range(wide))
    bias, term = action_terms(
        order, xh * sets + z, keyboard, mouse, key_table, mouse_table, weight_t
    )
    shares = [share_attention(own, s, rows, sets, outs) for s in (share, other_share)]
    part = guide(guidance, own, bias, term, shares, rows, outs)
    returned = lax.all_to_all(part, ("xh", "z"), 0, 0, tiled=True)
    mine = jnp.sum(returned.astype(F32), axis=0)
    other = lax.ppermute(mine, "branch", swap)
    both = jnp.where(core == 0, jnp.stack([mine, other]), jnp.stack([other, mine]))

    def laid(tokens):
        return tokens.reshape(2, 2, -1, outs).transpose(0, 2, 1, 3).reshape(-1, 2 * outs)

    velocity = both.reshape(2, -1, 2, outs).transpose(0, 2, 1, 3).reshape(-1, outs)
    stepped = (laid(latent) - step_size * both.reshape(-1, 2 * outs)).astype(BF)
    places = ("xh", "xl", "z")
    count = wide * narrow * sets
    index = jnp.stack([(xh * narrow + xl) * sets + z, jnp.int32(count)])
    before = lax.ppermute(stepped, places, [(i, i + 1) for i in range(count - 1)])
    after = lax.ppermute(stepped, places, [(i + 1, i) for i in range(count - 1)])
    taps_in = conv_in.reshape(conv_in.shape[0], -1, conv_in.shape[3])
    taps_out = conv_out.transpose(1, 0, 3, 2).reshape(3, -1, conv_out.shape[2])
    taps_out = jnp.pad(taps_out, ((0, 0), (0, 16 - taps_out.shape[1]), (0, 0)))
    taps_out = taps_out.reshape(-1, conv_out.shape[2])
    colours = decode(index, before, stepped, after, taps_in, gain[None], taps_out)
    return (velocity, colours)


def solution(mesh):
    cores = mesh.shape["branch"]
    tok = mesh.shape["tok"]

    def run(*arrays):
        heads = arrays[0].shape[1] // HEAD_DIM
        sets = heads // cores
        fine = Mesh(
            mesh.devices.reshape(mesh.shape["groups"], cores, cores, tok // heads, sets),
            ("groups", "branch", "xh", "xl", "z"),
        )
        tokens = P(("groups", "xh", "xl", "z"), None)
        placed = (
            tokens,
            tokens,
            tokens,
            P("groups"),
            P("groups"),
            P(),
            P(),
            P(),
            P(),
            tokens,
            P(),
            P(),
            P(),
        )
        return jax.shard_map(
            shards,
            mesh=fine,
            in_specs=placed,
            out_specs=(tokens, P(None, ("groups", "xh", "xl", "z"), None)),
            check_vma=False,
        )(*arrays)

    return run
```

```python
import functools
import math

import jax
import jax.numpy as jnp
from jax import lax
from jax.experimental import pallas as pl
from jax.experimental.pallas import tpu as pltpu
from jax.sharding import Mesh
from jax.sharding import PartitionSpec as P

HEAD_DIM = 128

step_size = 0.25
norm_eps = 1e-06
TO_EXP2 = HEAD_DIM ** (-0.5) / math.log(2.0)
BF = jnp.bfloat16
F32 = jnp.float32
VMEM = pl.BlockSpec(memory_space=pltpu.VMEM)
SMEM = pl.BlockSpec(memory_space=pltpu.SMEM)
GRANT = pltpu.CompilerParams(vmem_limit_bytes=12 << 20)


def in_hbm(array):
    return pltpu.with_memory_space_constraint(array, pltpu.HBM)


def dot(a, b, dims, **kw):
    return lax.dot_general(a, b, (dims, ((), ())), preferred_element_type=F32, **kw)


def pack_kernel(core_ref, q_ref, k_ref, v_ref, w_ref, out_ref, q_tmp, k_tmp, v_tmp, w_tmp, sems):
    heads, _, hd = out_ref.shape
    rows = q_tmp.shape[0]
    half = rows // 2
    mine = pl.ds(pl.multiple_of(core_ref[0] * rows, rows), rows)
    copies = [
        pltpu.make_async_copy(w_ref, w_tmp, sems.at[0]),
        pltpu.make_async_copy(v_ref.at[mine, :], v_tmp, sems.at[1]),
        pltpu.make_async_copy(q_ref.at[mine, :], q_tmp, sems.at[2]),
        pltpu.make_async_copy(k_ref.at[mine, :], k_tmp, sems.at[3]),
    ]
    for copy in copies:
        copy.start()
    for copy in copies:
        copy.wait()
    for h in range(heads):
        cols = slice(h * hd, (h + 1) * hd)
        out_ref[h, 0:rows, :] = q_tmp[:, cols]
        out_ref[h, rows : 2 * rows, :] = k_tmp[:, cols]
        projected = dot(v_tmp[:, cols], w_tmp[:, cols], ((1,), (1,)))
        projected = jnp.concatenate([projected[:half], projected[half:]], axis=1)
        out_ref[h, 2 * rows :, :] = projected.astype(BF)


def pack(core, queries, keys, values, weight_t, rows):
    width = queries.shape[1]
    heads = width // HEAD_DIM
    hbm = pl.BlockSpec(memory_space=pltpu.HBM)
    return pl.pallas_call(
        pack_kernel,
        in_specs=[SMEM, hbm, hbm, hbm, hbm],
        out_specs=VMEM,
        out_shape=jax.ShapeDtypeStruct((heads, 2 * rows + rows // 2, HEAD_DIM), BF),
        scratch_shapes=[pltpu.VMEM((rows, width), BF)] * 3
        + [pltpu.VMEM(weight_t.shape, BF), pltpu.SemaphoreType.DMA((4,))],
        name="pack",
        compiler_params=GRANT,
    )(core[None], *(in_hbm(a) for a in (queries, keys, values, weight_t)))


def terms_kernel(order, kb_ref, ms_ref, head_ref, key_ref, mouse_ref, w_ref, bias_ref, term_ref):
    rows_key = jnp.concatenate([key_ref[pl.ds(kb_ref[f], 1)] for f in order], axis=0)
    rows_mouse = jnp.concatenate([mouse_ref[pl.ds(ms_ref[f], 1)] for f in order], axis=0)
    rows_key = rows_key.astype(F32)
    rows_mouse = rows_mouse.astype(F32)
    bias_key, bias_mouse = rows_key[:, 0, :], rows_mouse[:, 0, :]
    bias = [bias_key + bias_mouse, bias_mouse, bias_key, jnp.zeros_like(bias_key)]
    bias_ref[...] = jnp.concatenate(bias, axis=0).astype(BF)
    terms = jnp.concatenate([rows_key[:, 1, :], rows_mouse[:, 1, :]], axis=0).astype(BF)
    term_ref[...] = dot(terms, w_ref[...], ((1,), (1,)))


def action_terms(order, head, keyboard, mouse, key_table, mouse_table, weight_t):
    frames = len(order)
    outs = weight_t.shape[0]
    return pl.pallas_call(
        functools.partial(terms_kernel, order),
        grid_spec=pltpu.PrefetchScalarGridSpec(
            num_scalar_prefetch=3,
            grid=(1,),
            in_specs=[
                pl.BlockSpec(key_table.shape[:2] + (HEAD_DIM,), lambda i, a, b, h: (0, 0, h[0])),
                pl.BlockSpec(mouse_table.shape[:2] + (HEAD_DIM,), lambda i, a, b, h: (0, 0, h[0])),
                pl.BlockSpec((outs, HEAD_DIM), lambda i, a, b, h: (0, h[0])),
            ],
            out_specs=[VMEM, VMEM],
        ),
        out_shape=[
            jax.ShapeDtypeStruct((4 * frames, HEAD_DIM), BF),
            jax.ShapeDtypeStruct((2 * frames, outs), F32),
        ],
        name="terms",
        compiler_params=GRANT,
    )(keyboard, mouse, head[None], key_table, mouse_table, weight_t)


def share_kernel(rows, sets, own_ref, share_ref, sum_ref, top_ref, total_ref):
    heads, _, hd = own_ref.shape
    half = rows // 2
    outs = sum_ref.shape[1]
    query = own_ref[:, 0:rows, :].reshape(heads * rows, hd)
    gathered, per_gather = share_ref.shape[0], heads // sets
    for at in range(gathered):
        for part in range(per_gather):
            frame = at * per_gather + part
            place = slice(part * sets, (part + 1) * sets)
            keys = share_ref[at, place, 0:rows, :].reshape(sets * rows, hd)
            values = share_ref[at, place, rows:, :].reshape(sets * half, hd)
            scores = dot(keys, query, ((1,), (1,)))
            top = jnp.max(scores, axis=0, keepdims=True)
            raised = jnp.exp2((scores - top) * TO_EXP2)
            top_ref[frame : frame + 1, :] = top
            total_ref[frame : frame + 1, :] = jnp.sum(raised, axis=0, keepdims=True)
            raised = raised.reshape(sets, 2, half, -1)
            low = raised[:, 0].reshape(sets * half, -1).astype(BF)
            high = raised[:, 1].reshape(sets * half, -1).astype(BF)
            summed = dot(values[:, :outs], low, ((0,), (0,)))
            sum_ref[frame] = summed + dot(values[:, outs:], high, ((0,), (0,)))


def share_attention(own, share, rows, sets, outs):
    heads = own.shape[0]
    tokens = heads * rows
    frames = share.shape[0] * heads // sets
    keys = frames * sets * rows
    return pl.pallas_call(
        functools.partial(share_kernel, rows, sets),
        in_specs=[VMEM, VMEM],
        out_specs=[VMEM, VMEM, VMEM],
        out_shape=[
            jax.ShapeDtypeStruct((frames, outs, tokens), F32),
            jax.ShapeDtypeStruct((frames, tokens), F32),
            jax.ShapeDtypeStruct((frames, tokens), F32),
        ],
        cost_estimate=pl.CostEstimate(
            flops=2 * tokens * keys * (HEAD_DIM + outs),
            transcendentals=tokens * keys,
            bytes_accessed=1 << 20,
        ),
        name="share",
        compiler_params=GRANT,
    )(own, share)


def guide_kernel(rows, guide_ref, own_ref, bias_ref, term_ref, *refs):
    shares, out_ref = refs[:-1], refs[-1]
    sum_refs, top_refs, total_refs = shares[0::3], shares[1::3], shares[2::3]
    heads, _, hd = own_ref.shape
    half = rows // 2
    count = top_refs[0].shape[0]
    query = own_ref[:, 0:rows, :].reshape(heads * rows, hd)
    shift = dot(bias_ref[...], query, ((1,), (1,)))
    tops = [r[...] for r in top_refs]
    totals = [r[...] for r in total_refs]
    mixes = [None] * len(tops)
    by_key, by_mouse = None, None
    for b in range(4):
        heights = [(top + shift[b * count : (b + 1) * count]) * TO_EXP2 for top in tops]
        peak = functools.reduce(jnp.maximum, heights)
        peak = jnp.max(peak, axis=0, keepdims=True)
        factors = [jnp.exp2(height - peak) for height in heights]
        loads = functools.reduce(jnp.add, [f * t for f, t in zip(factors, totals)])
        scale = guide_ref[b] / jnp.sum(loads, axis=0, keepdims=True)
        parts = [f * scale for f in factors]
        mixes = [p if m is None else m + p for m, p in zip(mixes, parts)]
        loads = loads * scale
        if b % 2 == 0:
            by_key = loads if by_key is None else by_key + loads
        if b < 2:
            by_mouse = loads if by_mouse is None else by_mouse + loads
    loads = jnp.concatenate([by_key, by_mouse], axis=0)
    result = dot(term_ref[...], loads, ((0,), (0,)), precision=lax.Precision.HIGHEST)
    for mix, sum_ref in zip(mixes, sum_refs):
        for frame in range(count):
            result = result + mix[frame : frame + 1, :] * sum_ref[frame]
    by_token = jnp.transpose(result).reshape(heads, 2, half, -1)
    packed = jnp.concatenate([by_token[:, 0], by_token[:, 1]], axis=2)
    out_ref[...] = packed.astype(BF)


def guide(guidance, own, bias, term, shares, rows, outs):
    heads = own.shape[0]
    arrays = [array for share in shares for array in share]
    return pl.pallas_call(
        functools.partial(guide_kernel, rows),
        in_specs=[SMEM] + [VMEM] * (3 + len(arrays)),
        out_specs=VMEM,
        out_shape=jax.ShapeDtypeStruct((heads, rows // 2, 2 * outs), BF),
        name="guide",
        compiler_params=GRANT,
    )(guidance, own, bias, term, *arrays)


def decode_kernel(index_ref, before_ref, mine_ref, after_ref, conv_in_ref, gain_ref, conv_out_ref, out_ref):
    outs = before_ref.shape[1] // 2
    lat = outs // 4
    tokens = before_ref.shape[0] * 2
    left, right = [], []
    for ref in (before_ref, mine_ref, after_ref):
        both = ref[...].astype(F32)
        quarter = tokens // 4
        parts = [both[:quarter], both[quarter:]]
        parts = [p[:, side] for p in parts for side in (slice(0, outs), slice(outs, None))]
        block = jnp.concatenate(parts, axis=0)
        edge = jnp.zeros_like(block[:1])
        earlier = jnp.concatenate([edge, block[:-1]], axis=0)
        later = jnp.concatenate([block[1:], edge], axis=0)
        for dy in range(2):
            at = 2 * lat * dy
            here = block[:, at : at + 2 * lat]
            left.append(jnp.concatenate([earlier[:, at + lat : at + 2 * lat], here], axis=1))
            right.append(jnp.concatenate([here, later[:, at : at + lat]], axis=1))
    height = 4 * tokens
    row = lax.broadcasted_iota(jnp.int32, (height, 1), 0) // tokens
    first, last = index_ref[0] == 0, index_ref[0] == index_ref[1] - 1
    keep = jnp.where((row == 0) & first | (row == 3) & last, 0.0, 1.0)
    taps = []
    for windows in (left, right):
        stack = jnp.concatenate(windows, axis=0).astype(BF)
        features = dot(stack[:height], conv_in_ref[0], ((1,), (0,)))
        for a in range(1, 3):
            part = stack[a * tokens : a * tokens + height]
            features = features + dot(part, conv_in_ref[a], ((1,), (0,)))
        power = jnp.mean(features * features, axis=1, keepdims=True)
        scaled = features * lax.rsqrt(power + norm_eps) * gain_ref[...]
        normed = scaled / (1.0 + jnp.exp(-scaled)) * keep
        taps.append(dot(conv_out_ref[...], normed.astype(BF), ((1,), (1,))))
    even, odd = taps
    step = even.shape[0] // 3
    lane = lax.broadcasted_iota(jnp.int32, (step, height), 1) % tokens
    before = jnp.where(lane == 0, 0.0, pltpu.roll(odd[:step], 1, 1))
    after = jnp.where(lane == tokens - 1, 0.0, pltpu.roll(even[2 * step :], height - 1, 1))
    columns = [
        before + even[step : 2 * step] + odd[2 * step :],
        even[:step] + odd[step : 2 * step] + after,
    ]
    source = lax.broadcasted_iota(jnp.int32, (height, height), 0)
    target = lax.broadcasted_iota(jnp.int32, (height, height), 1)
    colours = None
    for dx, column in enumerate(columns):
        moved = column[0:3]
        for a in range(1, 3):
            moved = moved + pltpu.roll(column[3 * a : 3 * a + 3], height - a * tokens, 1)
        chosen = jnp.where(target == 2 * source + dx, 1.0, 0.0)
        placed = dot(moved, chosen, ((1,), (0,)), precision=lax.Precision.HIGHEST)
        colours = placed if colours is None else colours + placed
    out_ref[:, 0, :] = colours[:, : 2 * tokens]
    out_ref[:, 1, :] = colours[:, 2 * tokens :]


def decode(index, before, mine, after, conv_in, gain, conv_out):
    tokens = before.shape[0] * 2
    return pl.pallas_call(
        decode_kernel,
        in_specs=[SMEM] + [VMEM] * 6,
        out_specs=VMEM,
        out_shape=jax.ShapeDtypeStruct((3, 2, 2 * tokens), F32),
        name="decode",
        compiler_params=GRANT,
    )(index, before, mine, after, conv_in, gain, conv_out)


def shards(
    queries,
    keys,
    values,
    keyboard,
    mouse,
    key_table,
    mouse_table,
    guidance,
    out_weight,
    latent,
    conv_in,
    gain,
    conv_out,
):
    wide, narrow, sets = lax.axis_size("xh"), lax.axis_size("xl"), lax.axis_size("z")
    xh, xl, z = lax.axis_index("xh"), lax.axis_index("xl"), lax.axis_index("z")
    cores = lax.axis_size("branch")
    core = lax.axis_index("branch")
    outs = out_weight.shape[1]
    frames = keyboard.shape[0]
    assert frames == wide * narrow and cores == 2
    rows = queries.shape[0] // cores
    swap = [(0, 1), (1, 0)]

    weight_t = out_weight.T
    packed = pack(core, queries, keys, values, weight_t, rows)
    own = lax.all_to_all(packed, ("xh", "z"), 0, 0, tiled=True)
    share = lax.all_gather(own[:, rows:, :], "xl")
    other_share = lax.ppermute(share, "branch", swap)
    order = tuple(range(frames))
    bias, term = action_terms(
        order, xh * sets + z, keyboard, mouse, key_table, mouse_table, weight_t
    )
    shares = [share_attention(own, s, rows, sets, outs) for s in (share, other_share)]
    part = guide(guidance, own, bias, term, shares, rows, outs)
    returned = lax.all_to_all(part, ("xh", "z"), 0, 0, tiled=True)
    mine = jnp.sum(returned.astype(F32), axis=0)
    other = lax.ppermute(mine, "branch", swap)
    both = jnp.where(core == 0, jnp.stack([mine, other]), jnp.stack([other, mine]))

    def laid(tokens):
        return tokens.reshape(2, 2, -1, outs).transpose(0, 2, 1, 3).reshape(-1, 2 * outs)

    velocity = both.reshape(2, -1, 2, outs).transpose(0, 2, 1, 3).reshape(-1, outs)
    stepped = (laid(latent) - step_size * both.reshape(-1, 2 * outs)).astype(BF)
    places = ("xl", "xh", "z")
    count = wide * narrow * sets
    index = jnp.stack([(xl * wide + xh) * sets + z, jnp.int32(count)])
    before = lax.ppermute(stepped, places, [(i, i + 1) for i in range(count - 1)])
    after = lax.ppermute(stepped, places, [(i + 1, i) for i in range(count - 1)])
    taps_in = conv_in.reshape(conv_in.shape[0], -1, conv_in.shape[3])
    taps_out = conv_out.transpose(1, 0, 3, 2).reshape(3, -1, conv_out.shape[2])
    taps_out = jnp.pad(taps_out, ((0, 0), (0, 16 - taps_out.shape[1]), (0, 0)))
    taps_out = taps_out.reshape(-1, conv_out.shape[2])
    colours = decode(index, before, stepped, after, taps_in, gain[None], taps_out)
    return (velocity, colours)


def solution(mesh):
    cores = mesh.shape["branch"]
    tok = mesh.shape["tok"]

    def run(*arrays):
        heads = arrays[0].shape[1] // HEAD_DIM
        sets = heads // cores
        fine = Mesh(
            mesh.devices.reshape(mesh.shape["groups"], cores, tok // heads, cores, sets),
            ("groups", "branch", "xl", "xh", "z"),
        )
        tokens = P(("groups", "xl", "xh", "z"), None)
        placed = (
            tokens,
            tokens,
            tokens,
            P("groups"),
            P("groups"),
            P(),
            P(),
            P(),
            P(),
            tokens,
            P(),
            P(),
            P(),
        )
        return jax.shard_map(
            shards,
            mesh=fine,
            in_specs=placed,
            out_specs=(tokens, P(None, ("groups", "xl", "xh", "z"), None)),
            check_vma=False,
        )(*arrays)

    return run
```

```python
import functools
import math

import jax
import jax.numpy as jnp
from jax import lax
from jax.experimental import pallas as pl
from jax.experimental.pallas import tpu as pltpu
from jax.sharding import Mesh
from jax.sharding import PartitionSpec as P

HEAD_DIM = 128

step_size = 0.25
norm_eps = 1e-06
TO_EXP2 = HEAD_DIM ** (-0.5) / math.log(2.0)
BF = jnp.bfloat16
F32 = jnp.float32
VMEM = pl.BlockSpec(memory_space=pltpu.VMEM)
SMEM = pl.BlockSpec(memory_space=pltpu.SMEM)
GRANT = pltpu.CompilerParams(vmem_limit_bytes=12 << 20)


def in_hbm(array):
    return pltpu.with_memory_space_constraint(array, pltpu.HBM)


def dot(a, b, dims, **kw):
    return lax.dot_general(a, b, (dims, ((), ())), preferred_element_type=F32, **kw)


def pack_kernel(
    core_ref, head_ref, q_ref, k_ref, v_ref, w_ref, kb_ref, ms_ref, key_ref, mouse_ref, guide_ref,
    out_ref, bias_ref, term_ref, line_ref,
    q_tmp, k_tmp, v_tmp, w_tmp, kb_tmp, ms_tmp, key_tmp, mouse_tmp, guide_tmp, sems,
):
    heads, _, hd = out_ref.shape
    rows = q_tmp.shape[0]
    half = rows // 2
    frames = kb_tmp.shape[0]
    mine = pl.ds(pl.multiple_of(core_ref[0] * rows, rows), rows)
    head = pl.ds(pl.multiple_of(head_ref[0] * hd, hd), hd)
    ids = [
        pltpu.make_async_copy(kb_ref, kb_tmp, sems.at[4]),
        pltpu.make_async_copy(ms_ref, ms_tmp, sems.at[5]),
        pltpu.make_async_copy(guide_ref, guide_tmp, sems.at[6]),
    ]
    copies = [
        pltpu.make_async_copy(w_ref, w_tmp, sems.at[0]),
        pltpu.make_async_copy(v_ref.at[mine, :], v_tmp, sems.at[1]),
        pltpu.make_async_copy(q_ref.at[mine, :], q_tmp, sems.at[2]),
        pltpu.make_async_copy(k_ref.at[mine, :], k_tmp, sems.at[3]),
    ]
    for copy in ids + copies:
        copy.start()
    for copy in ids:
        copy.wait()
    picks = []
    for f in range(frames):
        at = 7 + 2 * f
        picks += [
            pltpu.make_async_copy(key_ref.at[kb_tmp[f], :, head], key_tmp.at[f], sems.at[at]),
            pltpu.make_async_copy(mouse_ref.at[ms_tmp[f], :, head], mouse_tmp.at[f], sems.at[at + 1]),
        ]
    for copy in picks:
        copy.start()
    for copy in copies:
        copy.wait()
    for h in range(heads):
        cols = slice(h * hd, (h + 1) * hd)
        out_ref[h, 0:rows, :] = q_tmp[:, cols]
        out_ref[h, rows : 2 * rows, :] = k_tmp[:, cols]
        projected = dot(v_tmp[:, cols], w_tmp[:, cols], ((1,), (1,)))
        projected = jnp.concatenate([projected[:half], projected[half:]], axis=1)
        out_ref[h, 2 * rows :, :] = projected.astype(BF)
    for copy in picks:
        copy.wait()
    rows_key = key_tmp[...].astype(F32)
    rows_mouse = mouse_tmp[...].astype(F32)
    bias_key, bias_mouse = rows_key[:, 0, :], rows_mouse[:, 0, :]
    bias = [bias_key + bias_mouse, bias_mouse, bias_key, jnp.zeros_like(bias_key)]
    bias_ref[...] = jnp.concatenate(bias, axis=0).astype(BF)
    terms = jnp.concatenate([rows_key[:, 1, :], rows_mouse[:, 1, :]], axis=0).astype(BF)
    term_ref[...] = dot(terms, w_tmp[:, head], ((1,), (1,)))
    for b in range(line_ref.shape[0]):
        line_ref[b : b + 1, :] = jnp.full((1, hd), guide_tmp[b], F32)


def pack(
    core, head, queries, keys, values, weight_t, keyboard, mouse, key_table, mouse_table, guidance, rows
):
    width = queries.shape[1]
    heads = width // HEAD_DIM
    frames = keyboard.shape[0]
    outs = weight_t.shape[0]
    arrays = (queries, keys, values, weight_t, keyboard, mouse, key_table, mouse_table, guidance)
    return pl.pallas_call(
        pack_kernel,
        in_specs=[SMEM, SMEM] + [pl.BlockSpec(memory_space=pltpu.HBM)] * len(arrays),
        out_specs=[VMEM] * 4,
        out_shape=[
            jax.ShapeDtypeStruct((heads, 2 * rows + rows // 2, HEAD_DIM), BF),
            jax.ShapeDtypeStruct((4 * frames, HEAD_DIM), BF),
            jax.ShapeDtypeStruct((2 * frames, outs), F32),
            jax.ShapeDtypeStruct((guidance.shape[0], HEAD_DIM), F32),
        ],
        scratch_shapes=[pltpu.VMEM((rows, width), BF)] * 3
        + [pltpu.VMEM(weight_t.shape, BF)]
        + [pltpu.SMEM((frames,), jnp.int32)] * 2
        + [pltpu.VMEM((frames, 2, HEAD_DIM), BF)] * 2
        + [pltpu.SMEM(guidance.shape, F32)]
        + [pltpu.SemaphoreType.DMA((7 + 2 * frames,))],
        name="pack",
        compiler_params=GRANT,
    )(core[None], head[None], *(in_hbm(a) for a in arrays))


def share_kernel(rows, sets, own_ref, share_ref, sum_ref, top_ref, total_ref):
    heads, _, hd = own_ref.shape
    half = rows // 2
    outs = sum_ref.shape[1]
    query = own_ref[:, 0:rows, :].reshape(heads * rows, hd)
    per_gather = heads // sets
    frames = share_ref.shape[0] * per_gather

    def scores_of(frame):
        at, part = frame // per_gather, frame % per_gather
        keys = share_ref[at, part * sets : (part + 1) * sets, 0:rows, :]
        return dot(keys.reshape(sets * rows, hd), query, ((1,), (1,)))

    coming = scores_of(0)
    for frame in range(frames):
        scores = coming
        if frame + 1 < frames:
            coming = scores_of(frame + 1)
        at, part = frame // per_gather, frame % per_gather
        values = share_ref[at, part * sets : (part + 1) * sets, rows:, :].reshape(sets * half, hd)
        values = jnp.concatenate([values[:, :outs], values[:, outs:]], axis=0)
        top = jnp.max(scores, axis=0, keepdims=True)
        raised = jnp.exp2((scores - top) * TO_EXP2)
        top_ref[frame : frame + 1, :] = top
        total_ref[frame : frame + 1, :] = jnp.sum(raised, axis=0, keepdims=True)
        raised = raised.reshape(sets, 2, half, -1)
        low = raised[:, 0].reshape(sets * half, -1)
        high = raised[:, 1].reshape(sets * half, -1)
        raised = jnp.concatenate([low, high], axis=0).astype(BF)
        sum_ref[frame] = dot(values, raised, ((0,), (0,)))


def share_attention(own, share, rows, sets, outs):
    heads = own.shape[0]
    tokens = heads * rows
    frames = share.shape[0] * heads // sets
    keys = frames * sets * rows
    return pl.pallas_call(
        functools.partial(share_kernel, rows, sets),
        in_specs=[VMEM, VMEM],
        out_specs=[VMEM, VMEM, VMEM],
        out_shape=[
            jax.ShapeDtypeStruct((frames, outs, tokens), F32),
            jax.ShapeDtypeStruct((frames, tokens), F32),
            jax.ShapeDtypeStruct((frames, tokens), F32),
        ],
        cost_estimate=pl.CostEstimate(
            flops=2 * tokens * keys * (HEAD_DIM + outs),
            transcendentals=tokens * keys,
            bytes_accessed=1 << 20,
        ),
        name="share",
        compiler_params=GRANT,
    )(own, share)


def guide_kernel(rows, guide_ref, own_ref, bias_ref, term_ref, *refs):
    shares, out_ref = refs[:-1], refs[-1]
    sum_refs, top_refs, total_refs = shares[0::3], shares[1::3], shares[2::3]
    heads, _, hd = own_ref.shape
    half = rows // 2
    count = top_refs[0].shape[0]
    query = own_ref[:, 0:rows, :].reshape(heads * rows, hd)
    shift = dot(bias_ref[...], query, ((1,), (1,)))
    tops = [r[...] for r in top_refs]
    totals = [r[...] for r in total_refs]
    mixes = [None] * len(tops)
    by_key, by_mouse = None, None
    for b in range(4):
        heights = [(top + shift[b * count : (b + 1) * count]) * TO_EXP2 for top in tops]
        peak = functools.reduce(jnp.maximum, heights)
        peak = jnp.max(peak, axis=0, keepdims=True)
        factors = [jnp.exp2(height - peak) for height in heights]
        loads = functools.reduce(jnp.add, [f * t for f, t in zip(factors, totals)])
        scale = guide_ref[b : b + 1, 0:1] / jnp.sum(loads, axis=0, keepdims=True)
        parts = [f * scale for f in factors]
        mixes = [p if m is None else m + p for m, p in zip(mixes, parts)]
        loads = loads * scale
        if b % 2 == 0:
            by_key = loads if by_key is None else by_key + loads
        if b < 2:
            by_mouse = loads if by_mouse is None else by_mouse + loads
    loads = jnp.concatenate([by_key, by_mouse], axis=0)
    result = dot(term_ref[...], loads, ((0,), (0,)), precision=lax.Precision.HIGHEST)
    for mix, sum_ref in zip(mixes, sum_refs):
        for frame in range(count):
            result = result + mix[frame : frame + 1, :] * sum_ref[frame]
    by_token = jnp.transpose(result).reshape(heads, 2, half, -1)
    packed = jnp.concatenate([by_token[:, 0], by_token[:, 1]], axis=2)
    out_ref[...] = packed.astype(BF)


def guide(guidance, own, bias, term, shares, rows, outs):
    heads = own.shape[0]
    arrays = [array for share in shares for array in share]
    return pl.pallas_call(
        functools.partial(guide_kernel, rows),
        in_specs=[VMEM] * (4 + len(arrays)),
        out_specs=VMEM,
        out_shape=jax.ShapeDtypeStruct((heads, rows // 2, 2 * outs), BF),
        name="guide",
        compiler_params=GRANT,
    )(guidance, own, bias, term, *arrays)


def decode_kernel(index_ref, before_ref, mine_ref, after_ref, conv_in_ref, gain_ref, conv_out_ref, out_ref):
    outs = before_ref.shape[1] // 2
    lat = outs // 4
    tokens = before_ref.shape[0] * 2
    left, right = [], []
    for ref in (before_ref, mine_ref, after_ref):
        both = ref[...].astype(F32)
        quarter = tokens // 4
        parts = [both[:quarter], both[quarter:]]
        parts = [p[:, side] for p in parts for side in (slice(0, outs), slice(outs, None))]
        block = jnp.concatenate(parts, axis=0)
        edge = jnp.zeros_like(block[:1])
        earlier = jnp.concatenate([edge, block[:-1]], axis=0)
        later = jnp.concatenate([block[1:], edge], axis=0)
        for dy in range(2):
            at = 2 * lat * dy
            here = block[:, at : at + 2 * lat]
            left.append(jnp.concatenate([earlier[:, at + lat : at + 2 * lat], here], axis=1))
            right.append(jnp.concatenate([here, later[:, at : at + lat]], axis=1))
    height = 4 * tokens
    row = lax.broadcasted_iota(jnp.int32, (height, 1), 0) // tokens
    first, last = index_ref[0] == 0, index_ref[0] == index_ref[1] - 1
    keep = jnp.where((row == 0) & first | (row == 3) & last, 0.0, 1.0)
    taps = []
    for windows in (left, right):
        stack = jnp.concatenate(windows, axis=0).astype(BF)
        features = dot(stack[:height], conv_in_ref[0], ((1,), (0,)))
        for a in range(1, 3):
            part = stack[a * tokens : a * tokens + height]
            features = features + dot(part, conv_in_ref[a], ((1,), (0,)))
        power = jnp.mean(features * features, axis=1, keepdims=True)
        scaled = features * lax.rsqrt(power + norm_eps) * gain_ref[...]
        normed = scaled / (1.0 + jnp.exp(-scaled)) * keep
        taps.append(dot(conv_out_ref[...], normed.astype(BF), ((1,), (1,))))
    even, odd = taps
    step = even.shape[0] // 3
    lane = lax.broadcasted_iota(jnp.int32, (step, height), 1) % tokens
    before = jnp.where(lane == 0, 0.0, pltpu.roll(odd[:step], 1, 1))
    after = jnp.where(lane == tokens - 1, 0.0, pltpu.roll(even[2 * step :], height - 1, 1))
    columns = [
        before + even[step : 2 * step] + odd[2 * step :],
        even[:step] + odd[step : 2 * step] + after,
    ]
    source = lax.broadcasted_iota(jnp.int32, (height, height), 0)
    target = lax.broadcasted_iota(jnp.int32, (height, height), 1)
    colours = None
    for dx, column in enumerate(columns):
        moved = column[0:3]
        for a in range(1, 3):
            moved = moved + pltpu.roll(column[3 * a : 3 * a + 3], height - a * tokens, 1)
        chosen = jnp.where(target == 2 * source + dx, 1.0, 0.0)
        placed = dot(moved, chosen, ((1,), (0,)), precision=lax.Precision.HIGHEST)
        colours = placed if colours is None else colours + placed
    out_ref[:, 0, :] = colours[:, : 2 * tokens]
    out_ref[:, 1, :] = colours[:, 2 * tokens :]


def decode(index, before, mine, after, conv_in, gain, conv_out):
    tokens = before.shape[0] * 2
    return pl.pallas_call(
        decode_kernel,
        in_specs=[SMEM] + [VMEM] * 6,
        out_specs=VMEM,
        out_shape=jax.ShapeDtypeStruct((3, 2, 2 * tokens), F32),
        name="decode",
        compiler_params=GRANT,
    )(index, before, mine, after, conv_in, gain, conv_out)


def shards(
    queries,
    keys,
    values,
    keyboard,
    mouse,
    key_table,
    mouse_table,
    guidance,
    out_weight,
    latent,
    conv_in,
    gain,
    conv_out,
):
    wide, narrow, sets = lax.axis_size("xh"), lax.axis_size("xl"), lax.axis_size("z")
    xh, xl, z = lax.axis_index("xh"), lax.axis_index("xl"), lax.axis_index("z")
    cores = lax.axis_size("branch")
    core = lax.axis_index("branch")
    outs = out_weight.shape[1]
    assert keyboard.shape[0] == wide * narrow and cores == 2
    rows = queries.shape[0] // cores
    swap = [(0, 1), (1, 0)]

    weight_t = out_weight.T
    packed, bias, term, lines = pack(
        core, xh * sets + z, queries, keys, values, weight_t,
        keyboard, mouse, key_table, mouse_table, guidance, rows,
    )
    own = lax.all_to_all(packed, ("xh", "z"), 0, 0, tiled=True)
    share = lax.all_gather(own[:, rows:, :], "xl")
    other_share = lax.ppermute(share, "branch", swap)
    shares = [share_attention(own, s, rows, sets, outs) for s in (share, other_share)]
    part = guide(lines, own, bias, term, shares, rows, outs)
    part, latent, conv_out, gain = lax.optimization_barrier((part, latent, conv_out, gain))
    returned = lax.all_to_all(part, ("xh", "z"), 0, 0, tiled=True)

    def laid(tokens):
        return tokens.reshape(2, 2, -1, outs).transpose(0, 2, 1, 3).reshape(-1, 2 * outs)

    count = wide * narrow * sets
    index = jnp.stack([(xl * wide + xh) * sets + z, jnp.int32(count)])
    taps_in = conv_in.reshape(conv_in.shape[0], -1, conv_in.shape[3])
    taps_out = conv_out.transpose(1, 0, 3, 2).reshape(3, -1, conv_out.shape[2])
    taps_out = jnp.pad(taps_out, ((0, 0), (0, 16 - taps_out.shape[1]), (0, 0)))
    taps_out = taps_out.reshape(-1, conv_out.shape[2])
    noisy = laid(latent)
    mine = jnp.sum(returned.astype(F32), axis=0)
    mine, noisy, taps_out, gain, index = lax.optimization_barrier(
        (mine, noisy, taps_out, gain[None], index)
    )
    other = lax.ppermute(mine, "branch", swap)
    both = jnp.where(core == 0, jnp.stack([mine, other]), jnp.stack([other, mine]))
    velocity = both.reshape(2, -1, 2, outs).transpose(0, 2, 1, 3).reshape(-1, outs)
    stepped = (noisy - step_size * both.reshape(-1, 2 * outs)).astype(BF)
    places = ("xl", "xh", "z")
    before = lax.ppermute(stepped, places, [(i, i + 1) for i in range(count - 1)])
    after = lax.ppermute(stepped, places, [(i + 1, i) for i in range(count - 1)])
    colours = decode(index, before, stepped, after, taps_in, gain, taps_out)
    return (velocity, colours)


def solution(mesh):
    cores = mesh.shape["branch"]
    tok = mesh.shape["tok"]

    def run(*arrays):
        heads = arrays[0].shape[1] // HEAD_DIM
        sets = heads // cores
        fine = Mesh(
            mesh.devices.reshape(mesh.shape["groups"], cores, tok // heads, cores, sets),
            ("groups", "branch", "xl", "xh", "z"),
        )
        tokens = P(("groups", "xl", "xh", "z"), None)
        placed = (
            tokens,
            tokens,
            tokens,
            P("groups"),
            P("groups"),
            P(),
            P(),
            P(),
            P(),
            tokens,
            P(),
            P(),
            P(),
        )
        return jax.shard_map(
            shards,
            mesh=fine,
            in_specs=placed,
            out_specs=(tokens, P(None, ("groups", "xl", "xh", "z"), None)),
            check_vma=False,
        )(*arrays)

    return run
```

```python
import functools
import math

import jax
import jax.numpy as jnp
from jax import lax
from jax.experimental import pallas as pl
from jax.experimental.pallas import tpu as pltpu
from jax.sharding import Mesh
from jax.sharding import PartitionSpec as P

HEAD_DIM = 128

step_size = 0.25
norm_eps = 1e-06
TO_EXP2 = HEAD_DIM ** (-0.5) / math.log(2.0)
BF = jnp.bfloat16
F32 = jnp.float32
VMEM = pl.BlockSpec(memory_space=pltpu.VMEM)
SMEM = pl.BlockSpec(memory_space=pltpu.SMEM)
GRANT = pltpu.CompilerParams(vmem_limit_bytes=12 << 20)


def in_hbm(array):
    return pltpu.with_memory_space_constraint(array, pltpu.HBM)


def dot(a, b, dims, **kw):
    return lax.dot_general(a, b, (dims, ((), ())), preferred_element_type=F32, **kw)


def pack_kernel(
    core_ref, head_ref, q_ref, k_ref, v_ref, w_ref, kb_ref, ms_ref, key_ref, mouse_ref, guide_ref,
    out_ref, bias_ref, term_ref, line_ref,
    q_tmp, k_tmp, v_tmp, w_tmp, kb_tmp, ms_tmp, key_tmp, mouse_tmp, guide_tmp, sems,
):
    heads, _, hd = out_ref.shape
    rows = q_tmp.shape[0]
    half = rows // 2
    frames = kb_tmp.shape[0]
    mine = pl.ds(pl.multiple_of(core_ref[0] * rows, rows), rows)
    head = pl.ds(pl.multiple_of(head_ref[0] * hd, hd), hd)
    ids = [
        pltpu.make_async_copy(kb_ref, kb_tmp, sems.at[4]),
        pltpu.make_async_copy(ms_ref, ms_tmp, sems.at[5]),
        pltpu.make_async_copy(guide_ref, guide_tmp, sems.at[6]),
    ]
    copies = [
        pltpu.make_async_copy(w_ref, w_tmp, sems.at[0]),
        pltpu.make_async_copy(v_ref.at[mine, :], v_tmp, sems.at[1]),
        pltpu.make_async_copy(q_ref.at[mine, :], q_tmp, sems.at[2]),
        pltpu.make_async_copy(k_ref.at[mine, :], k_tmp, sems.at[3]),
    ]
    for copy in ids + copies:
        copy.start()
    for copy in ids:
        copy.wait()
    picks = []
    for f in range(frames):
        at = 7 + 2 * f
        picks += [
            pltpu.make_async_copy(key_ref.at[kb_tmp[f], :, head], key_tmp.at[f], sems.at[at]),
            pltpu.make_async_copy(mouse_ref.at[ms_tmp[f], :, head], mouse_tmp.at[f], sems.at[at + 1]),
        ]
    for copy in picks:
        copy.start()
    for copy in copies:
        copy.wait()
    for h in range(heads):
        cols = slice(h * hd, (h + 1) * hd)
        out_ref[h, 0:rows, :] = q_tmp[:, cols]
        out_ref[h, rows : 2 * rows, :] = k_tmp[:, cols]
        projected = dot(v_tmp[:, cols], w_tmp[:, cols], ((1,), (1,)))
        projected = jnp.concatenate([projected[:half], projected[half:]], axis=1)
        out_ref[h, 2 * rows :, :] = projected.astype(BF)
    for copy in picks:
        copy.wait()
    rows_key = key_tmp[...].astype(F32)
    rows_mouse = mouse_tmp[...].astype(F32)
    bias_key, bias_mouse = rows_key[:, 0, :], rows_mouse[:, 0, :]
    bias = [bias_key + bias_mouse, bias_mouse, bias_key, jnp.zeros_like(bias_key)]
    bias_ref[...] = jnp.concatenate(bias, axis=0).astype(BF)
    terms = jnp.concatenate([rows_key[:, 1, :], rows_mouse[:, 1, :]], axis=0).astype(BF)
    term_ref[...] = dot(terms, w_tmp[:, head], ((1,), (1,)))
    for b in range(line_ref.shape[0]):
        line_ref[b : b + 1, :] = jnp.full((1, hd), guide_tmp[b], F32)


def pack(
    core, head, queries, keys, values, weight_t, keyboard, mouse, key_table, mouse_table, guidance, rows
):
    width = queries.shape[1]
    heads = width // HEAD_DIM
    frames = keyboard.shape[0]
    outs = weight_t.shape[0]
    arrays = (queries, keys, values, weight_t, keyboard, mouse, key_table, mouse_table, guidance)
    return pl.pallas_call(
        pack_kernel,
        in_specs=[SMEM, SMEM] + [pl.BlockSpec(memory_space=pltpu.HBM)] * len(arrays),
        out_specs=[VMEM] * 4,
        out_shape=[
            jax.ShapeDtypeStruct((heads, 2 * rows + rows // 2, HEAD_DIM), BF),
            jax.ShapeDtypeStruct((4 * frames, HEAD_DIM), BF),
            jax.ShapeDtypeStruct((2 * frames, outs), F32),
            jax.ShapeDtypeStruct((guidance.shape[0], HEAD_DIM), F32),
        ],
        scratch_shapes=[pltpu.VMEM((rows, width), BF)] * 3
        + [pltpu.VMEM(weight_t.shape, BF)]
        + [pltpu.SMEM((frames,), jnp.int32)] * 2
        + [pltpu.VMEM((frames, 2, HEAD_DIM), BF)] * 2
        + [pltpu.SMEM(guidance.shape, F32)]
        + [pltpu.SemaphoreType.DMA((7 + 2 * frames,))],
        name="pack",
        compiler_params=GRANT,
    )(core[None], head[None], *(in_hbm(a) for a in arrays))


def share_body(rows, sets, heads, query, share_ref, sum_ref, top_ref, total_ref):
    hd = query.shape[1]
    half = rows // 2
    outs = sum_ref.shape[1]
    per_gather = heads // sets
    frames = share_ref.shape[0] * per_gather

    def scores_of(frame):
        at, part = frame // per_gather, frame % per_gather
        keys = share_ref[at, part * sets : (part + 1) * sets, 0:rows, :]
        return dot(keys.reshape(sets * rows, hd), query, ((1,), (1,)))

    coming = scores_of(0)
    for frame in range(frames):
        scores = coming
        if frame + 1 < frames:
            coming = scores_of(frame + 1)
        at, part = frame // per_gather, frame % per_gather
        values = share_ref[at, part * sets : (part + 1) * sets, rows:, :].reshape(sets * half, hd)
        values = jnp.concatenate([values[:, :outs], values[:, outs:]], axis=0)
        top = jnp.max(scores, axis=0, keepdims=True)
        raised = jnp.exp2((scores - top) * TO_EXP2)
        top_ref[frame : frame + 1, :] = top
        total_ref[frame : frame + 1, :] = jnp.sum(raised, axis=0, keepdims=True)
        raised = raised.reshape(sets, 2, half, -1)
        low = raised[:, 0].reshape(sets * half, -1)
        high = raised[:, 1].reshape(sets * half, -1)
        raised = jnp.concatenate([low, high], axis=0).astype(BF)
        sum_ref[frame] = dot(values, raised, ((0,), (0,)))


def own_share_kernel(rows, sets, at_ref, own_ref, share_ref, query_ref, *out_refs):
    heads, _, hd = own_ref.shape
    count = share_ref.shape[0]
    before, after = lax.rem(at_ref[0] + (count - 1), count), lax.rem(at_ref[0] + 1, count)
    earlier = share_ref[pl.ds(before, 1), heads + 1, 0:rows, :].reshape(rows, hd)
    later = share_ref[pl.ds(after, 1), heads, 0:rows, :].reshape(rows, hd)
    query = own_ref[:, 0:rows, :].reshape(heads * rows, hd)
    query_ref[0:rows, :] = earlier
    query_ref[rows : rows + heads * rows, :] = query
    query_ref[rows + heads * rows :, :] = later
    share_body(rows, sets, heads, query_ref[...], share_ref, *out_refs)


def other_share_kernel(rows, sets, heads, query_ref, share_ref, *out_refs):
    share_body(rows, sets, heads, query_ref[...], share_ref, *out_refs)


def share_shapes(share, heads, rows, sets, outs):
    tokens = (heads + 2) * rows
    frames = share.shape[0] * heads // sets
    shapes = [
        jax.ShapeDtypeStruct((frames, outs, tokens), F32),
        jax.ShapeDtypeStruct((frames, tokens), F32),
        jax.ShapeDtypeStruct((frames, tokens), F32),
    ]
    keys = frames * sets * rows
    cost = pl.CostEstimate(
        flops=2 * tokens * keys * (HEAD_DIM + outs),
        transcendentals=tokens * keys,
        bytes_accessed=1 << 20,
    )
    return tokens, shapes, cost


def own_share_attention(place, own, share, rows, sets, outs):
    tokens, shapes, cost = share_shapes(share, own.shape[0], rows, sets, outs)
    return pl.pallas_call(
        functools.partial(own_share_kernel, rows, sets),
        in_specs=[SMEM, VMEM, VMEM],
        out_specs=[VMEM] * 4,
        out_shape=[jax.ShapeDtypeStruct((tokens, HEAD_DIM), BF)] + shapes,
        cost_estimate=cost,
        name="own_share",
        compiler_params=GRANT,
    )(place[None], own, share)


def other_share_attention(query, share, heads, rows, sets, outs):
    _, shapes, cost = share_shapes(share, heads, rows, sets, outs)
    return pl.pallas_call(
        functools.partial(other_share_kernel, rows, sets, heads),
        in_specs=[VMEM, VMEM],
        out_specs=[VMEM] * 3,
        out_shape=shapes,
        cost_estimate=cost,
        name="other_share",
        compiler_params=GRANT,
    )(query, share)


def guide_kernel(rows, guide_ref, query_ref, bias_ref, term_ref, *refs):
    shares, out_ref = refs[:-1], refs[-1]
    sum_refs, top_refs, total_refs = shares[0::3], shares[1::3], shares[2::3]
    heads = out_ref.shape[0]
    half = rows // 2
    count = top_refs[0].shape[0]
    shift = dot(bias_ref[...], query_ref[...], ((1,), (1,)))
    tops = [r[...] for r in top_refs]
    totals = [r[...] for r in total_refs]
    mixes = [None] * len(tops)
    by_key, by_mouse = None, None
    for b in range(4):
        heights = [(top + shift[b * count : (b + 1) * count]) * TO_EXP2 for top in tops]
        peak = functools.reduce(jnp.maximum, heights)
        peak = jnp.max(peak, axis=0, keepdims=True)
        factors = [jnp.exp2(height - peak) for height in heights]
        loads = functools.reduce(jnp.add, [f * t for f, t in zip(factors, totals)])
        scale = guide_ref[b : b + 1, 0:1] / jnp.sum(loads, axis=0, keepdims=True)
        parts = [f * scale for f in factors]
        mixes = [p if m is None else m + p for m, p in zip(mixes, parts)]
        loads = loads * scale
        if b % 2 == 0:
            by_key = loads if by_key is None else by_key + loads
        if b < 2:
            by_mouse = loads if by_mouse is None else by_mouse + loads
    loads = jnp.concatenate([by_key, by_mouse], axis=0)
    result = dot(term_ref[...], loads, ((0,), (0,)), precision=lax.Precision.HIGHEST)
    for mix, sum_ref in zip(mixes, sum_refs):
        for frame in range(count):
            result = result + mix[frame : frame + 1, :] * sum_ref[frame]
    by_token = jnp.transpose(result).reshape(heads + 2, 2, half, -1)
    packed = jnp.concatenate([by_token[:, 0], by_token[:, 1]], axis=2).astype(BF)
    for side in range(3):
        out_ref[:, side * half : (side + 1) * half, :] = packed[side : side + heads]


def guide(lines, query, bias, term, shares, rows, outs):
    heads = query.shape[0] // rows - 2
    arrays = [array for share in shares for array in share]
    return pl.pallas_call(
        functools.partial(guide_kernel, rows),
        in_specs=[VMEM] * (4 + len(arrays)),
        out_specs=VMEM,
        out_shape=jax.ShapeDtypeStruct((heads, 3 * (rows // 2), 2 * outs), BF),
        name="guide",
        compiler_params=GRANT,
    )(lines, query, bias, term, *arrays)


def decode_kernel(
    index_ref, mine_ref, other_ref, noisy_ref, conv_in_ref, gain_ref, conv_out_ref, velocity_ref, out_ref
):
    outs = velocity_ref.shape[1]
    lat = outs // 4
    tokens = velocity_ref.shape[0]
    quarter = tokens // 4
    first, last = index_ref[0] == 0, index_ref[0] == index_ref[1] - 1
    low_core = index_ref[2] == 0
    left, right = [], []
    for side in range(3):
        place = slice(side * quarter, (side + 1) * quarter)
        here, there = mine_ref[place, :], other_ref[place, :]
        both = [jnp.where(low_core, here, there), jnp.where(low_core, there, here)]
        blocks = []
        for n, velocity in enumerate(both):
            stepped = noisy_ref[side, n * quarter : (n + 1) * quarter, :] - step_size * velocity
            blocks += [stepped[:, :outs], stepped[:, outs:]]
            if side == 1:
                at = 2 * n * quarter
                velocity_ref[at : at + quarter, :] = velocity[:, :outs]
                velocity_ref[at + quarter : at + 2 * quarter, :] = velocity[:, outs:]
        block = jnp.concatenate(blocks, axis=0).astype(BF).astype(F32)
        if side != 1:
            block = jnp.where(first if side == 0 else last, 0.0, block)
        edge = jnp.zeros_like(block[:1])
        earlier = jnp.concatenate([edge, block[:-1]], axis=0)
        later = jnp.concatenate([block[1:], edge], axis=0)
        for dy in range(2):
            at = 2 * lat * dy
            here = block[:, at : at + 2 * lat]
            left.append(jnp.concatenate([earlier[:, at + lat : at + 2 * lat], here], axis=1))
            right.append(jnp.concatenate([here, later[:, at : at + lat]], axis=1))
    height = 4 * tokens
    row = lax.broadcasted_iota(jnp.int32, (height, 1), 0) // tokens
    keep = jnp.where((row == 0) & first | (row == 3) & last, 0.0, 1.0)
    taps = []
    for windows in (left, right):
        stack = jnp.concatenate(windows, axis=0).astype(BF)
        features = dot(stack[:height], conv_in_ref[0], ((1,), (0,)))
        for a in range(1, 3):
            part = stack[a * tokens : a * tokens + height]
            features = features + dot(part, conv_in_ref[a], ((1,), (0,)))
        power = jnp.mean(features * features, axis=1, keepdims=True)
        scaled = features * lax.rsqrt(power + norm_eps) * gain_ref[...]
        normed = scaled / (1.0 + jnp.exp(-scaled)) * keep
        taps.append(dot(conv_out_ref[...], normed.astype(BF), ((1,), (1,))))
    even, odd = taps
    step = even.shape[0] // 3
    lane = lax.broadcasted_iota(jnp.int32, (step, height), 1) % tokens
    before = jnp.where(lane == 0, 0.0, pltpu.roll(odd[:step], 1, 1))
    after = jnp.where(lane == tokens - 1, 0.0, pltpu.roll(even[2 * step :], height - 1, 1))
    columns = [
        before + even[step : 2 * step] + odd[2 * step :],
        even[:step] + odd[step : 2 * step] + after,
    ]
    source = lax.broadcasted_iota(jnp.int32, (height, height), 0)
    target = lax.broadcasted_iota(jnp.int32, (height, height), 1)
    colours = None
    for dx, column in enumerate(columns):
        moved = column[0:3]
        for a in range(1, 3):
            moved = moved + pltpu.roll(column[3 * a : 3 * a + 3], height - a * tokens, 1)
        chosen = jnp.where(target == 2 * source + dx, 1.0, 0.0)
        placed = dot(moved, chosen, ((1,), (0,)), precision=lax.Precision.HIGHEST)
        colours = placed if colours is None else colours + placed
    out_ref[:, 0, :] = colours[:, : 2 * tokens]
    out_ref[:, 1, :] = colours[:, 2 * tokens :]


def decode(index, mine, other, noisy, conv_in, gain, conv_out):
    tokens, outs = 2 * noisy.shape[1], noisy.shape[2] // 2
    return pl.pallas_call(
        decode_kernel,
        in_specs=[SMEM] + [VMEM] * 6,
        out_specs=[VMEM, VMEM],
        out_shape=[
            jax.ShapeDtypeStruct((tokens, outs), F32),
            jax.ShapeDtypeStruct((3, 2, 2 * tokens), F32),
        ],
        name="decode",
        compiler_params=GRANT,
    )(index, mine, other, noisy, conv_in, gain, conv_out)


def shards(
    queries,
    keys,
    values,
    keyboard,
    mouse,
    key_table,
    mouse_table,
    guidance,
    out_weight,
    latent,
    conv_in,
    gain,
    conv_out,
):
    wide, narrow, sets = lax.axis_size("xh"), lax.axis_size("xl"), lax.axis_size("z")
    xh, xl, z = lax.axis_index("xh"), lax.axis_index("xl"), lax.axis_index("z")
    cores = lax.axis_size("branch")
    core = lax.axis_index("branch")
    outs = out_weight.shape[1]
    assert keyboard.shape[0] == wide * narrow and cores == 2
    rows = queries.shape[0] // cores
    swap = [(0, 1), (1, 0)]

    weight_t = out_weight.T
    packed, bias, term, lines = pack(
        core, xh * sets + z, queries, keys, values, weight_t,
        keyboard, mouse, key_table, mouse_table, guidance, rows,
    )
    own = lax.all_to_all(packed, ("xh", "z"), 0, 0, tiled=True)
    moving = jnp.concatenate(
        [own[:, rows:], own[:1, : rows + rows // 2], own[-1:, : rows + rows // 2]], axis=0
    )
    share = lax.all_gather(moving, "xl")
    other_share = lax.ppermute(share, "branch", swap)
    query, *first = own_share_attention(xl, own, share, rows, sets, outs)
    second = other_share_attention(query, other_share, own.shape[0], rows, sets, outs)
    part = guide(lines, query, bias, term, [first, second], rows, outs)
    part, latent, conv_out, gain = lax.optimization_barrier((part, latent, conv_out, gain))
    returned = lax.all_to_all(part, ("xh", "z"), 0, 0, tiled=True)

    count = wide * narrow * sets
    places = ("xl", "xh", "z")
    index = jnp.stack([(xl * wide + xh) * sets + z, jnp.int32(count), core])
    taps_in = conv_in.reshape(conv_in.shape[0], -1, conv_in.shape[3])
    taps_out = conv_out.transpose(1, 0, 3, 2).reshape(3, -1, conv_out.shape[2])
    taps_out = jnp.pad(taps_out, ((0, 0), (0, 16 - taps_out.shape[1]), (0, 0)))
    taps_out = taps_out.reshape(-1, conv_out.shape[2])
    noisy = latent.reshape(2, 2, -1, outs).transpose(0, 2, 1, 3).reshape(-1, 2 * outs)
    before = lax.ppermute(noisy, places, [(i, i + 1) for i in range(count - 1)])
    after = lax.ppermute(noisy, places, [(i + 1, i) for i in range(count - 1)])
    noisy = jnp.stack([before, noisy, after])
    mine = jnp.sum(returned.astype(F32), axis=0)
    mine, noisy, taps_out, gain, index = lax.optimization_barrier(
        (mine, noisy, taps_out, gain[None], index)
    )
    other = lax.ppermute(mine, "branch", swap)
    return tuple(decode(index, mine, other, noisy, taps_in, gain, taps_out))


def solution(mesh):
    cores = mesh.shape["branch"]
    tok = mesh.shape["tok"]

    def run(*arrays):
        heads = arrays[0].shape[1] // HEAD_DIM
        sets = heads // cores
        fine = Mesh(
            mesh.devices.reshape(mesh.shape["groups"], cores, tok // heads, cores, sets),
            ("groups", "branch", "xl", "xh", "z"),
        )
        tokens = P(("groups", "xl", "xh", "z"), None)
        placed = (
            tokens,
            tokens,
            tokens,
            P("groups"),
            P("groups"),
            P(),
            P(),
            P(),
            P(),
            tokens,
            P(),
            P(),
            P(),
        )
        return jax.shard_map(
            shards,
            mesh=fine,
            in_specs=placed,
            out_specs=(tokens, P(None, ("groups", "xl", "xh", "z"), None)),
            check_vma=False,
        )(*arrays)

    return run
```

```python
import functools
import math

import jax
import jax.numpy as jnp
from jax import lax
from jax.experimental import pallas as pl
from jax.experimental.pallas import tpu as pltpu
from jax.sharding import Mesh
from jax.sharding import PartitionSpec as P

HEAD_DIM = 128

step_size = 0.25
norm_eps = 1e-06
TO_EXP2 = HEAD_DIM ** (-0.5) / math.log(2.0)
BF = jnp.bfloat16
F32 = jnp.float32
VMEM = pl.BlockSpec(memory_space=pltpu.VMEM)
SMEM = pl.BlockSpec(memory_space=pltpu.SMEM)
GRANT = pltpu.CompilerParams(vmem_limit_bytes=12 << 20)


def in_hbm(array):
    return pltpu.with_memory_space_constraint(array, pltpu.HBM)


def dot(a, b, dims, **kw):
    return lax.dot_general(a, b, (dims, ((), ())), preferred_element_type=F32, **kw)


def pack_kernel(
    core_ref, head_ref, q_ref, k_ref, v_ref, w_ref, kb_ref, ms_ref, key_ref, mouse_ref, guide_ref,
    out_ref, bias_ref, term_ref, line_ref,
    q_tmp, k_tmp, v_tmp, w_tmp, kb_tmp, ms_tmp, key_tmp, mouse_tmp, guide_tmp, sems,
):
    heads, _, hd = out_ref.shape
    rows = q_tmp.shape[0]
    half = rows // 2
    frames = kb_tmp.shape[0]
    mine = pl.ds(pl.multiple_of(core_ref[0] * rows, rows), rows)
    head = pl.ds(pl.multiple_of(head_ref[0] * hd, hd), hd)
    ids = [
        pltpu.make_async_copy(kb_ref, kb_tmp, sems.at[4]),
        pltpu.make_async_copy(ms_ref, ms_tmp, sems.at[5]),
        pltpu.make_async_copy(guide_ref, guide_tmp, sems.at[6]),
    ]
    width = w_tmp.shape[1]
    cuts = [slice(n * width // 2, (n + 1) * width // 2) for n in range(2)]
    copies = [
        pltpu.make_async_copy(q_ref.at[mine, :], q_tmp, sems.at[0]),
        pltpu.make_async_copy(k_ref.at[mine, :], k_tmp, sems.at[1]),
        pltpu.make_async_copy(v_ref.at[mine, :], v_tmp, sems.at[2]),
        pltpu.make_async_copy(w_ref.at[:, cuts[0]], w_tmp.at[:, cuts[0]], sems.at[3]),
        pltpu.make_async_copy(w_ref.at[:, cuts[1]], w_tmp.at[:, cuts[1]], sems.at[7]),
    ]
    for copy in ids + copies:
        copy.start()
    for copy in ids:
        copy.wait()
    picks = []
    for f in range(frames):
        at = 8 + 2 * f
        picks += [
            pltpu.make_async_copy(key_ref.at[kb_tmp[f], :, head], key_tmp.at[f], sems.at[at]),
            pltpu.make_async_copy(mouse_ref.at[ms_tmp[f], :, head], mouse_tmp.at[f], sems.at[at + 1]),
        ]
    for copy in picks:
        copy.start()
    for copy in copies[:2]:
        copy.wait()
    for h in range(heads):
        cols = slice(h * hd, (h + 1) * hd)
        out_ref[h, 0:rows, :] = q_tmp[:, cols]
        out_ref[h, rows : 2 * rows, :] = k_tmp[:, cols]
    for copy in copies[2:4]:
        copy.wait()
    for h in range(heads):
        if h == heads // 2:
            copies[4].wait()
        cols = slice(h * hd, (h + 1) * hd)
        projected = dot(v_tmp[:, cols], w_tmp[:, cols], ((1,), (1,)))
        projected = jnp.concatenate([projected[:half], projected[half:]], axis=1)
        out_ref[h, 2 * rows :, :] = projected.astype(BF)
    for copy in picks:
        copy.wait()
    rows_key = key_tmp[...].astype(F32)
    rows_mouse = mouse_tmp[...].astype(F32)
    bias_key, bias_mouse = rows_key[:, 0, :], rows_mouse[:, 0, :]
    bias = [bias_key + bias_mouse, bias_mouse, bias_key, jnp.zeros_like(bias_key)]
    bias_ref[...] = jnp.concatenate(bias, axis=0).astype(BF)
    terms = jnp.concatenate([rows_key[:, 1, :], rows_mouse[:, 1, :]], axis=0).astype(BF)
    term_ref[...] = dot(terms, w_tmp[:, head], ((1,), (1,)))
    for b in range(line_ref.shape[0]):
        line_ref[b : b + 1, :] = jnp.full((1, hd), guide_tmp[b], F32)


def pack(
    core, head, queries, keys, values, weight_t, keyboard, mouse, key_table, mouse_table, guidance, rows
):
    width = queries.shape[1]
    heads = width // HEAD_DIM
    frames = keyboard.shape[0]
    outs = weight_t.shape[0]
    arrays = (queries, keys, values, weight_t, keyboard, mouse, key_table, mouse_table, guidance)
    return pl.pallas_call(
        pack_kernel,
        in_specs=[SMEM, SMEM] + [pl.BlockSpec(memory_space=pltpu.HBM)] * len(arrays),
        out_specs=[VMEM] * 4,
        out_shape=[
            jax.ShapeDtypeStruct((heads, 2 * rows + rows // 2, HEAD_DIM), BF),
            jax.ShapeDtypeStruct((4 * frames, HEAD_DIM), BF),
            jax.ShapeDtypeStruct((2 * frames, outs), F32),
            jax.ShapeDtypeStruct((guidance.shape[0], HEAD_DIM), F32),
        ],
        scratch_shapes=[pltpu.VMEM((rows, width), BF)] * 3
        + [pltpu.VMEM(weight_t.shape, BF)]
        + [pltpu.SMEM((frames,), jnp.int32)] * 2
        + [pltpu.VMEM((frames, 2, HEAD_DIM), BF)] * 2
        + [pltpu.SMEM(guidance.shape, F32)]
        + [pltpu.SemaphoreType.DMA((8 + 2 * frames,))],
        name="pack",
        compiler_params=GRANT,
    )(core[None], head[None], *(in_hbm(a) for a in arrays))


def share_body(rows, sets, heads, query, share_ref, sum_ref, top_ref, total_ref):
    hd = query.shape[1]
    half = rows // 2
    outs = sum_ref.shape[1]
    per_gather = heads // sets
    frames = share_ref.shape[0] * per_gather

    def scores_of(frame):
        at, part = frame // per_gather, frame % per_gather
        keys = share_ref[at, part * sets : (part + 1) * sets, 0:rows, :]
        return dot(keys.reshape(sets * rows, hd), query, ((1,), (1,)))

    coming = scores_of(0)
    for frame in range(frames):
        scores = coming
        if frame + 1 < frames:
            coming = scores_of(frame + 1)
        at, part = frame // per_gather, frame % per_gather
        values = share_ref[at, part * sets : (part + 1) * sets, rows:, :].reshape(sets * half, hd)
        values = jnp.concatenate([values[:, :outs], values[:, outs:]], axis=0)
        top = jnp.max(scores, axis=0, keepdims=True)
        raised = jnp.exp2((scores - top) * TO_EXP2)
        top_ref[frame : frame + 1, :] = top
        total_ref[frame : frame + 1, :] = jnp.sum(raised, axis=0, keepdims=True)
        raised = raised.reshape(sets, 2, half, -1)
        low = raised[:, 0].reshape(sets * half, -1)
        high = raised[:, 1].reshape(sets * half, -1)
        raised = jnp.concatenate([low, high], axis=0).astype(BF)
        sum_ref[frame] = dot(values, raised, ((0,), (0,)))


def own_share_kernel(rows, sets, at_ref, own_ref, share_ref, query_ref, *out_refs):
    heads, _, hd = own_ref.shape
    count = share_ref.shape[0]
    before, after = lax.rem(at_ref[0] + (count - 1), count), lax.rem(at_ref[0] + 1, count)
    earlier = share_ref[pl.ds(before, 1), heads + 1, 0:rows, :].reshape(rows, hd)
    later = share_ref[pl.ds(after, 1), heads, 0:rows, :].reshape(rows, hd)
    query = own_ref[:, 0:rows, :].reshape(heads * rows, hd)
    query_ref[0:rows, :] = earlier
    query_ref[rows : rows + heads * rows, :] = query
    query_ref[rows + heads * rows :, :] = later
    share_body(rows, sets, heads, query_ref[...], share_ref, *out_refs)


def other_share_kernel(rows, sets, heads, query_ref, share_ref, *out_refs):
    share_body(rows, sets, heads, query_ref[...], share_ref, *out_refs)


def share_shapes(share, heads, rows, sets, outs):
    tokens = (heads + 2) * rows
    frames = share.shape[0] * heads // sets
    shapes = [
        jax.ShapeDtypeStruct((frames, outs, tokens), F32),
        jax.ShapeDtypeStruct((frames, tokens), F32),
        jax.ShapeDtypeStruct((frames, tokens), F32),
    ]
    keys = frames * sets * rows
    cost = pl.CostEstimate(
        flops=2 * tokens * keys * (HEAD_DIM + outs),
        transcendentals=tokens * keys,
        bytes_accessed=1 << 20,
    )
    return tokens, shapes, cost


def own_share_attention(place, own, share, rows, sets, outs):
    tokens, shapes, cost = share_shapes(share, own.shape[0], rows, sets, outs)
    return pl.pallas_call(
        functools.partial(own_share_kernel, rows, sets),
        in_specs=[SMEM, VMEM, VMEM],
        out_specs=[VMEM] * 4,
        out_shape=[jax.ShapeDtypeStruct((tokens, HEAD_DIM), BF)] + shapes,
        cost_estimate=cost,
        name="own_share",
        compiler_params=GRANT,
    )(place[None], own, share)


def other_share_attention(query, share, heads, rows, sets, outs):
    _, shapes, cost = share_shapes(share, heads, rows, sets, outs)
    return pl.pallas_call(
        functools.partial(other_share_kernel, rows, sets, heads),
        in_specs=[VMEM, VMEM],
        out_specs=[VMEM] * 3,
        out_shape=shapes,
        cost_estimate=cost,
        name="other_share",
        compiler_params=GRANT,
    )(query, share)


def guide_kernel(rows, guide_ref, query_ref, bias_ref, term_ref, *refs):
    shares, out_ref = refs[:-1], refs[-1]
    sum_refs, top_refs, total_refs = shares[0::3], shares[1::3], shares[2::3]
    heads = out_ref.shape[0]
    half = rows // 2
    count = top_refs[0].shape[0]
    shift = dot(bias_ref[...], query_ref[...], ((1,), (1,)))
    tops = [r[...] for r in top_refs]
    totals = [r[...] for r in total_refs]
    mixes = [None] * len(tops)
    by_key, by_mouse = None, None
    for b in range(4):
        heights = [(top + shift[b * count : (b + 1) * count]) * TO_EXP2 for top in tops]
        peak = functools.reduce(jnp.maximum, heights)
        peak = jnp.max(peak, axis=0, keepdims=True)
        factors = [jnp.exp2(height - peak) for height in heights]
        loads = functools.reduce(jnp.add, [f * t for f, t in zip(factors, totals)])
        scale = guide_ref[b : b + 1, 0:1] / jnp.sum(loads, axis=0, keepdims=True)
        parts = [f * scale for f in factors]
        mixes = [p if m is None else m + p for m, p in zip(mixes, parts)]
        loads = loads * scale
        if b % 2 == 0:
            by_key = loads if by_key is None else by_key + loads
        if b < 2:
            by_mouse = loads if by_mouse is None else by_mouse + loads
    loads = jnp.concatenate([by_key, by_mouse], axis=0)
    result = dot(term_ref[...], loads, ((0,), (0,)), precision=lax.Precision.HIGHEST)
    for mix, sum_ref in zip(mixes, sum_refs):
        for frame in range(count):
            result = result + mix[frame : frame + 1, :] * sum_ref[frame]
    by_token = jnp.transpose(result).reshape(heads + 2, 2, half, -1)
    packed = jnp.concatenate([by_token[:, 0], by_token[:, 1]], axis=2).astype(BF)
    for side in range(3):
        out_ref[:, side * half : (side + 1) * half, :] = packed[side : side + heads]


def guide(lines, query, bias, term, shares, rows, outs):
    heads = query.shape[0] // rows - 2
    arrays = [array for share in shares for array in share]
    return pl.pallas_call(
        functools.partial(guide_kernel, rows),
        in_specs=[VMEM] * (4 + len(arrays)),
        out_specs=VMEM,
        out_shape=pltpu.VMEM((heads, 3 * (rows // 2), 2 * outs), BF),
        name="guide",
        compiler_params=GRANT,
    )(lines, query, bias, term, *arrays)


def decode_kernel(
    flag_ref, mine_ref, other_ref, noisy_ref, conv_in_ref, gain_ref, conv_out_ref,
    velocity_out, colours_out, velocity_ref, out_ref, sems,
):
    outs = velocity_ref.shape[1]
    lat = outs // 4
    tokens = velocity_ref.shape[0]
    quarter = tokens // 4
    first, last = flag_ref[0:1, 0:1] > 0.5, flag_ref[1:2, 0:1] > 0.5
    low_core = flag_ref[2:3, :] > 0.5
    left, right = [], []
    for side in range(3):
        place = slice(side * quarter, (side + 1) * quarter)
        here, there = mine_ref[place, :], other_ref[place, :]
        both = [jnp.where(low_core, here, there), jnp.where(low_core, there, here)]
        blocks = []
        for n, velocity in enumerate(both):
            stepped = noisy_ref[side, n * quarter : (n + 1) * quarter, :] - step_size * velocity
            blocks += [stepped[:, :outs], stepped[:, outs:]]
            if side == 1:
                at = 2 * n * quarter
                velocity_ref[at : at + quarter, :] = velocity[:, :outs]
                velocity_ref[at + quarter : at + 2 * quarter, :] = velocity[:, outs:]
        block = jnp.concatenate(blocks, axis=0).astype(BF).astype(F32)
        if side == 1:
            velocity_copy = pltpu.make_async_copy(velocity_ref, velocity_out, sems.at[0])
            velocity_copy.start()
        else:
            block = jnp.where(first if side == 0 else last, 0.0, block)
        edge = jnp.zeros_like(block[:1])
        earlier = jnp.concatenate([edge, block[:-1]], axis=0)
        later = jnp.concatenate([block[1:], edge], axis=0)
        for dy in range(2):
            at = 2 * lat * dy
            here = block[:, at : at + 2 * lat]
            left.append(jnp.concatenate([earlier[:, at + lat : at + 2 * lat], here], axis=1))
            right.append(jnp.concatenate([here, later[:, at : at + lat]], axis=1))
    height = 4 * tokens
    row = lax.broadcasted_iota(jnp.int32, (height, 1), 0) // tokens
    keep = jnp.where((row == 0) & first | (row == 3) & last, 0.0, 1.0)
    taps = []
    for windows in (left, right):
        stack = jnp.concatenate(windows, axis=0).astype(BF)
        features = dot(stack[:height], conv_in_ref[0], ((1,), (0,)))
        for a in range(1, 3):
            part = stack[a * tokens : a * tokens + height]
            features = features + dot(part, conv_in_ref[a], ((1,), (0,)))
        power = jnp.mean(features * features, axis=1, keepdims=True)
        scaled = features * lax.rsqrt(power + norm_eps) * gain_ref[...]
        normed = scaled / (1.0 + jnp.exp(-scaled)) * keep
        taps.append(dot(conv_out_ref[...], normed.astype(BF), ((1,), (1,))))
    even, odd = taps
    step = even.shape[0] // 3
    lane = lax.broadcasted_iota(jnp.int32, (step, height), 1) % tokens
    before = jnp.where(lane == 0, 0.0, pltpu.roll(odd[:step], 1, 1))
    after = jnp.where(lane == tokens - 1, 0.0, pltpu.roll(even[2 * step :], height - 1, 1))
    columns = [
        before + even[step : 2 * step] + odd[2 * step :],
        even[:step] + odd[step : 2 * step] + after,
    ]
    source = lax.broadcasted_iota(jnp.int32, (height, height), 0)
    target = lax.broadcasted_iota(jnp.int32, (height, height), 1)
    colours = None
    for dx, column in enumerate(columns):
        moved = column[0:3]
        for a in range(1, 3):
            moved = moved + pltpu.roll(column[3 * a : 3 * a + 3], height - a * tokens, 1)
        chosen = jnp.where(target == 2 * source + dx, 1.0, 0.0)
        placed = dot(moved, chosen, ((1,), (0,)), precision=lax.Precision.HIGHEST)
        colours = placed if colours is None else colours + placed
    out_ref[:, 0, :] = colours[:, : 2 * tokens]
    out_ref[:, 1, :] = colours[:, 2 * tokens :]
    colours_copy = pltpu.make_async_copy(out_ref, colours_out, sems.at[1])
    colours_copy.start()
    velocity_copy.wait()
    colours_copy.wait()


def decode(flags, mine, other, noisy, conv_in, gain, conv_out):
    tokens, outs = 2 * noisy.shape[1], noisy.shape[2] // 2
    return pl.pallas_call(
        decode_kernel,
        in_specs=[VMEM] * 7,
        out_specs=[pl.BlockSpec(memory_space=pltpu.HBM)] * 2,
        out_shape=[
            jax.ShapeDtypeStruct((tokens, outs), F32),
            jax.ShapeDtypeStruct((3, 2, 2 * tokens), F32),
        ],
        scratch_shapes=[
            pltpu.VMEM((tokens, outs), F32),
            pltpu.VMEM((3, 2, 2 * tokens), F32),
            pltpu.SemaphoreType.DMA((2,)),
        ],
        name="decode",
        compiler_params=GRANT,
    )(flags, mine, other, noisy, conv_in, gain, conv_out)


def shards(
    queries,
    keys,
    values,
    keyboard,
    mouse,
    key_table,
    mouse_table,
    guidance,
    out_weight,
    latent,
    conv_in,
    gain,
    conv_out,
):
    wide, narrow, sets = lax.axis_size("xh"), lax.axis_size("xl"), lax.axis_size("z")
    xh, xl, z = lax.axis_index("xh"), lax.axis_index("xl"), lax.axis_index("z")
    cores = lax.axis_size("branch")
    core = lax.axis_index("branch")
    outs = out_weight.shape[1]
    assert keyboard.shape[0] == wide * narrow and cores == 2
    rows = queries.shape[0] // cores
    swap = [(0, 1), (1, 0)]

    weight_t = out_weight.T
    packed, bias, term, lines = pack(
        core, xh * sets + z, queries, keys, values, weight_t,
        keyboard, mouse, key_table, mouse_table, guidance, rows,
    )
    own = lax.all_to_all(packed, ("xh", "z"), 0, 0, tiled=True)
    moving = jnp.concatenate(
        [own[:, rows:], own[:1, : rows + rows // 2], own[-1:, : rows + rows // 2]], axis=0
    )
    share = lax.all_gather(moving, "xl")
    other_share = lax.ppermute(share, "branch", swap)
    query, *first = own_share_attention(xl, own, share, rows, sets, outs)
    second = other_share_attention(query, other_share, own.shape[0], rows, sets, outs)
    part = guide(lines, query, bias, term, [first, second], rows, outs)
    part, latent, conv_out, gain = lax.optimization_barrier((part, latent, conv_out, gain))
    returned = lax.all_to_all(part, ("xh", "z"), 0, 0, tiled=True)

    count = wide * narrow * sets
    places = ("xl", "xh", "z")
    index = (xl * wide + xh) * sets + z
    line = lax.broadcasted_iota(jnp.int32, (8, HEAD_DIM), 0)
    flags = (line == 0) & (index == 0) | (line == 1) & (index == count - 1) | (line == 2) & (core == 0)
    flags = flags.astype(F32)
    taps_in = conv_in.reshape(conv_in.shape[0], -1, conv_in.shape[3])
    taps_out = conv_out.transpose(1, 0, 3, 2).reshape(3, -1, conv_out.shape[2])
    taps_out = jnp.pad(taps_out, ((0, 0), (0, 16 - taps_out.shape[1]), (0, 0)))
    taps_out = taps_out.reshape(-1, conv_out.shape[2])
    noisy = latent.reshape(2, 2, -1, outs).transpose(0, 2, 1, 3).reshape(-1, 2 * outs)
    before = lax.ppermute(noisy, places, [(i, i + 1) for i in range(count - 1)])
    after = lax.ppermute(noisy, places, [(i + 1, i) for i in range(count - 1)])
    noisy = jnp.stack([before, noisy, after])
    mine = jnp.sum(returned.astype(F32), axis=0)
    mine, noisy, taps_out, gain, flags = lax.optimization_barrier(
        (mine, noisy, taps_out, gain[None], flags)
    )
    other = lax.ppermute(mine, "branch", swap)
    return tuple(decode(flags, mine, other, noisy, taps_in, gain, taps_out))


def solution(mesh):
    cores = mesh.shape["branch"]
    tok = mesh.shape["tok"]

    def run(*arrays):
        heads = arrays[0].shape[1] // HEAD_DIM
        sets = heads // cores
        fine = Mesh(
            mesh.devices.reshape(mesh.shape["groups"], cores, tok // heads, cores, sets),
            ("groups", "branch", "xl", "xh", "z"),
        )
        tokens = P(("groups", "xl", "xh", "z"), None)
        placed = (
            tokens,
            tokens,
            tokens,
            P("groups"),
            P("groups"),
            P(),
            P(),
            P(),
            P(),
            tokens,
            P(),
            P(),
            P(),
        )
        return jax.shard_map(
            shards,
            mesh=fine,
            in_specs=placed,
            out_specs=(tokens, P(None, ("groups", "xl", "xh", "z"), None)),
            check_vma=False,
        )(*arrays)

    return run
```

```python
import functools
import math

import jax
import jax.numpy as jnp
from jax import lax
from jax.experimental import pallas as pl
from jax.experimental.pallas import tpu as pltpu
from jax.sharding import Mesh
from jax.sharding import PartitionSpec as P

HEAD_DIM = 128

step_size = 0.25
norm_eps = 1e-06
TO_EXP2 = HEAD_DIM ** (-0.5) / math.log(2.0)
BF = jnp.bfloat16
F32 = jnp.float32
VMEM = pl.BlockSpec(memory_space=pltpu.VMEM)
SMEM = pl.BlockSpec(memory_space=pltpu.SMEM)
HBM = pl.BlockSpec(memory_space=pltpu.HBM)
GRANT = pltpu.CompilerParams(vmem_limit_bytes=12 << 20)


def in_hbm(array):
    return pltpu.with_memory_space_constraint(array, pltpu.HBM)


def dot(a, b, dims, **kw):
    return lax.dot_general(a, b, (dims, ((), ())), preferred_element_type=F32, **kw)


def pack_kernel(core_ref, q_ref, k_ref, v_ref, w_ref, out_ref, q_tmp, k_tmp, v_tmp, w_tmp, sems):
    heads, _, hd = out_ref.shape
    rows = q_tmp.shape[0]
    half = rows // 2
    mine = pl.ds(pl.multiple_of(core_ref[0] * rows, rows), rows)
    copies = [
        pltpu.make_async_copy(q_ref.at[mine, :], q_tmp, sems.at[0]),
        pltpu.make_async_copy(k_ref.at[mine, :], k_tmp, sems.at[1]),
        pltpu.make_async_copy(v_ref.at[mine, :], v_tmp, sems.at[2]),
        pltpu.make_async_copy(w_ref, w_tmp, sems.at[3]),
    ]
    for copy in copies:
        copy.start()
    for source, first, copy in ((q_tmp, 0, copies[0]), (k_tmp, rows, copies[1])):
        copy.wait()
        for h in range(heads):
            out_ref[h, first : first + rows, :] = source[:, h * hd : (h + 1) * hd]
    for copy in copies[2:]:
        copy.wait()
    for h in range(heads):
        cols = slice(h * hd, (h + 1) * hd)
        projected = dot(v_tmp[:, cols], w_tmp[:, cols], ((1,), (1,)))
        projected = jnp.concatenate([projected[:half], projected[half:]], axis=1)
        out_ref[h, 2 * rows :, :] = projected.astype(BF)


def pack(core, queries, keys, values, weight_t, rows):
    width = queries.shape[1]
    heads = width // HEAD_DIM
    return pl.pallas_call(
        pack_kernel,
        in_specs=[SMEM] + [HBM] * 4,
        out_specs=VMEM,
        out_shape=jax.ShapeDtypeStruct((heads, 2 * rows + rows // 2, HEAD_DIM), BF),
        scratch_shapes=[pltpu.VMEM((rows, width), BF)] * 3
        + [pltpu.VMEM(weight_t.shape, BF), pltpu.SemaphoreType.DMA((4,))],
        name="pack",
        compiler_params=GRANT,
    )(core[None], *(in_hbm(a) for a in (queries, keys, values, weight_t)))


def share_body(rows, sets, heads, query, share_ref, sum_ref, top_ref, total_ref):
    hd = query.shape[1]
    half = rows // 2
    outs = sum_ref.shape[1]
    per_gather = heads // sets
    frames = share_ref.shape[0] * per_gather

    def scores_of(frame):
        at, part = frame // per_gather, frame % per_gather
        keys = share_ref[at, part * sets : (part + 1) * sets, 0:rows, :]
        return dot(keys.reshape(sets * rows, hd), query, ((1,), (1,)))

    coming = scores_of(0)
    for frame in range(frames):
        scores = coming
        if frame + 1 < frames:
            coming = scores_of(frame + 1)
        at, part = frame // per_gather, frame % per_gather
        values = share_ref[at, part * sets : (part + 1) * sets, rows:, :].reshape(sets * half, hd)
        values = jnp.concatenate([values[:, :outs], values[:, outs:]], axis=0)
        top = jnp.max(scores, axis=0, keepdims=True)
        raised = jnp.exp2((scores - top) * TO_EXP2)
        top_ref[frame : frame + 1, :] = top
        total_ref[frame : frame + 1, :] = jnp.sum(raised, axis=0, keepdims=True)
        raised = raised.reshape(sets, 2, half, -1)
        low = raised[:, 0].reshape(sets * half, -1)
        high = raised[:, 1].reshape(sets * half, -1)
        raised = jnp.concatenate([low, high], axis=0).astype(BF)
        sum_ref[frame] = dot(values, raised, ((0,), (0,)))


def own_share_kernel(
    rows, sets, at_ref, head_ref, own_ref, share_ref, w_ref, kb_ref, ms_ref, key_ref, mouse_ref, guide_ref,
    query_ref, sum_ref, top_ref, total_ref, bias_ref, term_ref, line_ref,
    w_tmp, kb_tmp, ms_tmp, key_tmp, mouse_tmp, guide_tmp, sems,
):
    heads, _, hd = own_ref.shape
    frames = kb_tmp.shape[0]
    head = pl.ds(pl.multiple_of(head_ref[0] * hd, hd), hd)
    ids = [
        pltpu.make_async_copy(kb_ref, kb_tmp, sems.at[0]),
        pltpu.make_async_copy(ms_ref, ms_tmp, sems.at[1]),
    ]
    picks = [
        pltpu.make_async_copy(guide_ref, guide_tmp, sems.at[2]),
        pltpu.make_async_copy(w_ref.at[:, head], w_tmp, sems.at[3]),
    ]
    for copy in ids + picks:
        copy.start()
    count = share_ref.shape[0]
    before, after = lax.rem(at_ref[0] + (count - 1), count), lax.rem(at_ref[0] + 1, count)
    earlier = share_ref[pl.ds(before, 1), heads + 1, 0:rows, :].reshape(rows, hd)
    later = share_ref[pl.ds(after, 1), heads, 0:rows, :].reshape(rows, hd)
    query = own_ref[:, 0:rows, :].reshape(heads * rows, hd)
    query_ref[0:rows, :] = earlier
    query_ref[rows : rows + heads * rows, :] = query
    query_ref[rows + heads * rows :, :] = later
    for copy in ids:
        copy.wait()
    for f in range(frames):
        at = 4 + 2 * f
        picks += [
            pltpu.make_async_copy(key_ref.at[kb_tmp[f], :, head], key_tmp.at[f], sems.at[at]),
            pltpu.make_async_copy(mouse_ref.at[ms_tmp[f], :, head], mouse_tmp.at[f], sems.at[at + 1]),
        ]
    for copy in picks[2:]:
        copy.start()
    share_body(rows, sets, heads, query_ref[...], share_ref, sum_ref, top_ref, total_ref)
    for copy in picks:
        copy.wait()
    rows_key = key_tmp[...].astype(F32)
    rows_mouse = mouse_tmp[...].astype(F32)
    bias_key, bias_mouse = rows_key[:, 0, :], rows_mouse[:, 0, :]
    bias = [bias_key + bias_mouse, bias_mouse, bias_key, jnp.zeros_like(bias_key)]
    bias_ref[...] = jnp.concatenate(bias, axis=0).astype(BF)
    terms = jnp.concatenate([rows_key[:, 1, :], rows_mouse[:, 1, :]], axis=0).astype(BF)
    term_ref[...] = dot(terms, w_tmp[...], ((1,), (1,)))
    for b in range(line_ref.shape[0]):
        line_ref[b : b + 1, :] = jnp.full((1, hd), guide_tmp[b], F32)


def share_shapes(share, heads, rows, sets, outs):
    tokens = (heads + 2) * rows
    frames = share.shape[0] * heads // sets
    shapes = [
        jax.ShapeDtypeStruct((frames, outs, tokens), F32),
        jax.ShapeDtypeStruct((frames, tokens), F32),
        jax.ShapeDtypeStruct((frames, tokens), F32),
    ]
    keys = frames * sets * rows
    cost = pl.CostEstimate(
        flops=2 * tokens * keys * (HEAD_DIM + outs),
        transcendentals=tokens * keys,
        bytes_accessed=1 << 20,
    )
    return tokens, shapes, cost


def own_share_attention(
    place, head, own, share, weight_t, keyboard, mouse, key_table, mouse_table, guidance, rows, sets
):
    outs = weight_t.shape[0]
    frames = keyboard.shape[0]
    tokens, shapes, cost = share_shapes(share, own.shape[0], rows, sets, outs)
    arrays = (weight_t, keyboard, mouse, key_table, mouse_table, guidance)
    return pl.pallas_call(
        functools.partial(own_share_kernel, rows, sets),
        in_specs=[SMEM, SMEM, VMEM, VMEM] + [HBM] * len(arrays),
        out_specs=[VMEM] * 7,
        out_shape=[jax.ShapeDtypeStruct((tokens, HEAD_DIM), BF)]
        + shapes
        + [
            jax.ShapeDtypeStruct((4 * frames, HEAD_DIM), BF),
            jax.ShapeDtypeStruct((2 * frames, outs), F32),
            jax.ShapeDtypeStruct((guidance.shape[0], HEAD_DIM), F32),
        ],
        scratch_shapes=[pltpu.VMEM((outs, HEAD_DIM), BF)]
        + [pltpu.SMEM((frames,), jnp.int32)] * 2
        + [pltpu.VMEM((frames, 2, HEAD_DIM), BF)] * 2
        + [pltpu.SMEM(guidance.shape, F32), pltpu.SemaphoreType.DMA((4 + 2 * frames,))],
        cost_estimate=cost,
        name="own_share",
        compiler_params=GRANT,
    )(place[None], head[None], own, share, *(in_hbm(a) for a in arrays))


def guide_kernel(rows, guide_ref, query_ref, bias_ref, term_ref, *refs):
    shares, out_ref = refs[:-1], refs[-1]
    sum_refs, top_refs, total_refs = shares[0::3], shares[1::3], shares[2::3]
    heads = out_ref.shape[0]
    half = rows // 2
    count = top_refs[0].shape[0]
    shift = dot(bias_ref[...], query_ref[...], ((1,), (1,)))
    tops = [r[...] for r in top_refs]
    totals = [r[...] for r in total_refs]
    mixes = [None] * len(tops)
    by_key, by_mouse = None, None
    for b in range(4):
        heights = [(top + shift[b * count : (b + 1) * count]) * TO_EXP2 for top in tops]
        peak = functools.reduce(jnp.maximum, heights)
        peak = jnp.max(peak, axis=0, keepdims=True)
        factors = [jnp.exp2(height - peak) for height in heights]
        loads = functools.reduce(jnp.add, [f * t for f, t in zip(factors, totals)])
        scale = guide_ref[b : b + 1, 0:1] / jnp.sum(loads, axis=0, keepdims=True)
        parts = [f * scale for f in factors]
        mixes = [p if m is None else m + p for m, p in zip(mixes, parts)]
        loads = loads * scale
        if b % 2 == 0:
            by_key = loads if by_key is None else by_key + loads
        if b < 2:
            by_mouse = loads if by_mouse is None else by_mouse + loads
    loads = jnp.concatenate([by_key, by_mouse], axis=0)
    result = dot(term_ref[...], loads, ((0,), (0,)), precision=lax.Precision.HIGHEST)
    for mix, sum_ref in zip(mixes, sum_refs):
        for frame in range(count):
            result = result + mix[frame : frame + 1, :] * sum_ref[frame]
    by_token = jnp.transpose(result).reshape(heads + 2, 2, half, -1)
    packed = jnp.concatenate([by_token[:, 0], by_token[:, 1]], axis=2).astype(BF)
    for side in range(3):
        out_ref[:, side * half : (side + 1) * half, :] = packed[side : side + heads]


def other_share_kernel(
    rows, sets, query_ref, share_ref, line_ref, bias_ref, term_ref,
    sum_ref, top_ref, total_ref, out_ref, sum_tmp, top_tmp, total_tmp,
):
    heads = out_ref.shape[0]
    share_body(rows, sets, heads, query_ref[...], share_ref, sum_tmp, top_tmp, total_tmp)
    shares = (sum_ref, top_ref, total_ref, sum_tmp, top_tmp, total_tmp)
    guide_kernel(rows, line_ref, query_ref, bias_ref, term_ref, *shares, out_ref)


def other_share_and_guide(query, share, lines, bias, term, first, rows, sets, outs):
    heads = query.shape[0] // rows - 2
    _, shapes, cost = share_shapes(share, heads, rows, sets, outs)
    return pl.pallas_call(
        functools.partial(other_share_kernel, rows, sets),
        in_specs=[VMEM] * 8,
        out_specs=VMEM,
        out_shape=jax.ShapeDtypeStruct((heads, 3 * (rows // 2), 2 * outs), BF),
        scratch_shapes=[pltpu.VMEM(a.shape, a.dtype) for a in shapes],
        cost_estimate=cost,
        name="other_share",
        compiler_params=GRANT,
    )(query, share, lines, bias, term, *first)


def decode_kernel(
    flag_ref, mine_ref, other_ref, noisy_ref, conv_in_ref, gain_ref, conv_out_ref,
    velocity_out, colours_out, velocity_ref, out_ref, sems,
):
    outs = velocity_ref.shape[1]
    lat = outs // 4
    tokens = velocity_ref.shape[0]
    quarter = tokens // 4
    first, last = flag_ref[0:1, 0:1] > 0.5, flag_ref[1:2, 0:1] > 0.5
    low_core = flag_ref[2:3, :] > 0.5
    left, right = [], []
    for side in range(3):
        place = slice(side * quarter, (side + 1) * quarter)
        here, there = mine_ref[place, :], other_ref[place, :]
        both = [jnp.where(low_core, here, there), jnp.where(low_core, there, here)]
        blocks = []
        for n, velocity in enumerate(both):
            stepped = noisy_ref[side, n * quarter : (n + 1) * quarter, :] - step_size * velocity
            blocks += [stepped[:, :outs], stepped[:, outs:]]
            if side == 1:
                at = 2 * n * quarter
                velocity_ref[at : at + quarter, :] = velocity[:, :outs]
                velocity_ref[at + quarter : at + 2 * quarter, :] = velocity[:, outs:]
        block = jnp.concatenate(blocks, axis=0).astype(BF).astype(F32)
        if side == 1:
            velocity_copy = pltpu.make_async_copy(velocity_ref, velocity_out, sems.at[0])
            velocity_copy.start()
        else:
            block = jnp.where(first if side == 0 else last, 0.0, block)
        edge = jnp.zeros_like(block[:1])
        earlier = jnp.concatenate([edge, block[:-1]], axis=0)
        later = jnp.concatenate([block[1:], edge], axis=0)
        for dy in range(2):
            at = 2 * lat * dy
            here = block[:, at : at + 2 * lat]
            left.append(jnp.concatenate([earlier[:, at + lat : at + 2 * lat], here], axis=1))
            right.append(jnp.concatenate([here, later[:, at : at + lat]], axis=1))
    height = 4 * tokens
    row = lax.broadcasted_iota(jnp.int32, (height, 1), 0) // tokens
    keep = jnp.where((row == 0) & first | (row == 3) & last, 0.0, 1.0)
    taps = []
    for windows in (left, right):
        stack = jnp.concatenate(windows, axis=0).astype(BF)
        features = dot(stack[:height], conv_in_ref[0], ((1,), (0,)))
        for a in range(1, 3):
            part = stack[a * tokens : a * tokens + height]
            features = features + dot(part, conv_in_ref[a], ((1,), (0,)))
        power = jnp.mean(features * features, axis=1, keepdims=True)
        scaled = features * lax.rsqrt(power + norm_eps) * gain_ref[...]
        normed = scaled / (1.0 + jnp.exp(-scaled)) * keep
        taps.append(dot(conv_out_ref[...], normed.astype(BF), ((1,), (1,))))
    even, odd = taps
    step = even.shape[0] // 3
    lane = lax.broadcasted_iota(jnp.int32, (step, height), 1) % tokens
    before = jnp.where(lane == 0, 0.0, pltpu.roll(odd[:step], 1, 1))
    after = jnp.where(lane == tokens - 1, 0.0, pltpu.roll(even[2 * step :], height - 1, 1))
    columns = [
        before + even[step : 2 * step] + odd[2 * step :],
        even[:step] + odd[step : 2 * step] + after,
    ]
    source = lax.broadcasted_iota(jnp.int32, (height, height), 0)
    target = lax.broadcasted_iota(jnp.int32, (height, height), 1)
    colours = None
    for dx, column in enumerate(columns):
        moved = column[0:3]
        for a in range(1, 3):
            moved = moved + pltpu.roll(column[3 * a : 3 * a + 3], height - a * tokens, 1)
        chosen = jnp.where(target == 2 * source + dx, 1.0, 0.0)
        placed = dot(moved, chosen, ((1,), (0,)), precision=lax.Precision.HIGHEST)
        colours = placed if colours is None else colours + placed
    out_ref[:, 0, :] = colours[:, : 2 * tokens]
    out_ref[:, 1, :] = colours[:, 2 * tokens :]
    colours_copy = pltpu.make_async_copy(out_ref, colours_out, sems.at[1])
    colours_copy.start()
    velocity_copy.wait()
    colours_copy.wait()


def decode(flags, mine, other, noisy, conv_in, gain, conv_out):
    tokens, outs = 2 * noisy.shape[1], noisy.shape[2] // 2
    return pl.pallas_call(
        decode_kernel,
        in_specs=[VMEM] * 7,
        out_specs=[pl.BlockSpec(memory_space=pltpu.HBM)] * 2,
        out_shape=[
            jax.ShapeDtypeStruct((tokens, outs), F32),
            jax.ShapeDtypeStruct((3, 2, 2 * tokens), F32),
        ],
        scratch_shapes=[
            pltpu.VMEM((tokens, outs), F32),
            pltpu.VMEM((3, 2, 2 * tokens), F32),
            pltpu.SemaphoreType.DMA((2,)),
        ],
        name="decode",
        compiler_params=GRANT,
    )(flags, mine, other, noisy, conv_in, gain, conv_out)


def shards(
    queries,
    keys,
    values,
    keyboard,
    mouse,
    key_table,
    mouse_table,
    guidance,
    out_weight,
    latent,
    conv_in,
    gain,
    conv_out,
):
    wide, narrow, sets = lax.axis_size("xh"), lax.axis_size("xl"), lax.axis_size("z")
    xh, xl, z = lax.axis_index("xh"), lax.axis_index("xl"), lax.axis_index("z")
    cores = lax.axis_size("branch")
    core = lax.axis_index("branch")
    outs = out_weight.shape[1]
    assert keyboard.shape[0] == wide * narrow and cores == 2
    rows = queries.shape[0] // cores
    swap = [(0, 1), (1, 0)]

    weight_t = out_weight.T
    packed = pack(core, queries, keys, values, weight_t, rows)
    own = lax.all_to_all(packed, ("xh", "z"), 0, 0, tiled=True)
    moving = jnp.concatenate(
        [own[:, rows:], own[:1, : rows + rows // 2], own[-1:, : rows + rows // 2]], axis=0
    )
    share = lax.all_gather(moving, "xl")
    other_share = lax.ppermute(share, "branch", swap)
    query, *first, bias, term, lines = own_share_attention(
        xl, xh * sets + z, own, share, weight_t,
        keyboard, mouse, key_table, mouse_table, guidance, rows, sets,
    )
    part = other_share_and_guide(query, other_share, lines, bias, term, first, rows, sets, outs)
    part, latent, conv_out, gain = lax.optimization_barrier((part, latent, conv_out, gain))
    returned = lax.all_to_all(part, ("xh", "z"), 0, 0, tiled=True)

    count = wide * narrow * sets
    places = ("xl", "xh", "z")
    index = (xl * wide + xh) * sets + z
    line = lax.broadcasted_iota(jnp.int32, (8, HEAD_DIM), 0)
    flags = (line == 0) & (index == 0) | (line == 1) & (index == count - 1) | (line == 2) & (core == 0)
    flags = flags.astype(F32)
    taps_in = conv_in.reshape(conv_in.shape[0], -1, conv_in.shape[3])
    taps_out = conv_out.transpose(1, 0, 3, 2).reshape(3, -1, conv_out.shape[2])
    taps_out = jnp.pad(taps_out, ((0, 0), (0, 16 - taps_out.shape[1]), (0, 0)))
    taps_out = taps_out.reshape(-1, conv_out.shape[2])
    noisy = latent.reshape(2, 2, -1, outs).transpose(0, 2, 1, 3).reshape(-1, 2 * outs)
    before = lax.ppermute(noisy, places, [(i, i + 1) for i in range(count - 1)])
    after = lax.ppermute(noisy, places, [(i + 1, i) for i in range(count - 1)])
    noisy = jnp.stack([before, noisy, after])
    mine = jnp.sum(returned.astype(F32), axis=0)
    mine, noisy, taps_out, gain, flags = lax.optimization_barrier(
        (mine, noisy, taps_out, gain[None], flags)
    )
    other = lax.ppermute(mine, "branch", swap)
    return tuple(decode(flags, mine, other, noisy, taps_in, gain, taps_out))


def solution(mesh):
    cores = mesh.shape["branch"]
    tok = mesh.shape["tok"]

    def run(*arrays):
        heads = arrays[0].shape[1] // HEAD_DIM
        sets = heads // cores
        fine = Mesh(
            mesh.devices.reshape(mesh.shape["groups"], cores, tok // heads, cores, sets),
            ("groups", "branch", "xl", "xh", "z"),
        )
        tokens = P(("groups", "xl", "xh", "z"), None)
        placed = (
            tokens,
            tokens,
            tokens,
            P("groups"),
            P("groups"),
            P(),
            P(),
            P(),
            P(),
            tokens,
            P(),
            P(),
            P(),
        )
        return jax.shard_map(
            shards,
            mesh=fine,
            in_specs=placed,
            out_specs=(tokens, P(None, ("groups", "xl", "xh", "z"), None)),
            check_vma=False,
        )(*arrays)

    return run
```

```python
import functools
import math

import jax
import jax.numpy as jnp
from jax import lax
from jax.experimental import pallas as pl
from jax.experimental.pallas import tpu as pltpu
from jax.sharding import Mesh
from jax.sharding import PartitionSpec as P

HEAD_DIM = 128

step_size = 0.25
norm_eps = 1e-06
TO_EXP2 = HEAD_DIM ** (-0.5) / math.log(2.0)
BF = jnp.bfloat16
F32 = jnp.float32
VMEM = pl.BlockSpec(memory_space=pltpu.VMEM)
SMEM = pl.BlockSpec(memory_space=pltpu.SMEM)
HBM = pl.BlockSpec(memory_space=pltpu.HBM)
GRANT = pltpu.CompilerParams(vmem_limit_bytes=12 << 20)


def in_hbm(array):
    return pltpu.with_memory_space_constraint(array, pltpu.HBM)


def dot(a, b, dims, **kw):
    return lax.dot_general(a, b, (dims, ((), ())), preferred_element_type=F32, **kw)


def pack_kernel(core_ref, q_ref, k_ref, v_ref, w_ref, out_ref, q_tmp, k_tmp, v_tmp, w_tmp, sems):
    heads, _, hd = out_ref.shape
    rows = q_tmp.shape[0]
    half = rows // 2
    mine = pl.ds(pl.multiple_of(core_ref[0] * rows, rows), rows)
    copies = [
        pltpu.make_async_copy(q_ref.at[mine, :], q_tmp, sems.at[0]),
        pltpu.make_async_copy(k_ref.at[mine, :], k_tmp, sems.at[1]),
        pltpu.make_async_copy(v_ref.at[mine, :], v_tmp, sems.at[2]),
        pltpu.make_async_copy(w_ref, w_tmp, sems.at[3]),
    ]
    for copy in copies:
        copy.start()
    for source, first, copy in ((q_tmp, 0, copies[0]), (k_tmp, rows, copies[1])):
        copy.wait()
        for h in range(heads):
            out_ref[h, first : first + rows, :] = source[:, h * hd : (h + 1) * hd]
    for copy in copies[2:]:
        copy.wait()
    for h in range(heads):
        cols = slice(h * hd, (h + 1) * hd)
        projected = dot(v_tmp[:, cols], w_tmp[:, cols], ((1,), (1,)))
        projected = jnp.concatenate([projected[:half], projected[half:]], axis=1)
        out_ref[h, 2 * rows :, :] = projected.astype(BF)


def pack(core, queries, keys, values, weight_t, rows):
    width = queries.shape[1]
    heads = width // HEAD_DIM
    return pl.pallas_call(
        pack_kernel,
        in_specs=[SMEM] + [HBM] * 4,
        out_specs=VMEM,
        out_shape=jax.ShapeDtypeStruct((heads, 2 * rows + rows // 2, HEAD_DIM), BF),
        scratch_shapes=[pltpu.VMEM((rows, width), BF)] * 3
        + [pltpu.VMEM(weight_t.shape, BF), pltpu.SemaphoreType.DMA((4,))],
        name="pack",
        compiler_params=GRANT,
    )(core[None], *(in_hbm(a) for a in (queries, keys, values, weight_t)))


def share_body(rows, sets, heads, query, share_ref, sum_ref, top_ref, total_ref, midway=None):
    hd = query.shape[1]
    half = rows // 2
    outs = sum_ref.shape[1]
    per_gather = heads // sets
    frames = share_ref.shape[0] * per_gather

    def scores_of(frame):
        at, part = frame // per_gather, frame % per_gather
        keys = share_ref[at, part * sets : (part + 1) * sets, 0:rows, :]
        return dot(keys.reshape(sets * rows, hd), query, ((1,), (1,)))

    coming = scores_of(0)
    for frame in range(frames):
        scores = coming
        if frame + 1 < frames:
            coming = scores_of(frame + 1)
        at, part = frame // per_gather, frame % per_gather
        values = share_ref[at, part * sets : (part + 1) * sets, rows:, :].reshape(sets * half, hd)
        values = jnp.concatenate([values[:, :outs], values[:, outs:]], axis=0)
        top = jnp.max(scores, axis=0, keepdims=True)
        raised = jnp.exp2((scores - top) * TO_EXP2)
        top_ref[frame : frame + 1, :] = top
        total_ref[frame : frame + 1, :] = jnp.sum(raised, axis=0, keepdims=True)
        raised = raised.reshape(sets, 2, half, -1)
        low = raised[:, 0].reshape(sets * half, -1)
        high = raised[:, 1].reshape(sets * half, -1)
        raised = jnp.concatenate([low, high], axis=0).astype(BF)
        sum_ref[frame] = dot(values, raised, ((0,), (0,)))
        if midway is not None and frame == frames // 2:
            midway()


def own_share_kernel(
    rows, sets, at_ref, head_ref, own_ref, share_ref, w_ref, kb_ref, ms_ref, key_ref, mouse_ref, guide_ref,
    query_ref, sum_ref, top_ref, total_ref, bias_ref, term_ref, line_ref,
    w_tmp, kb_tmp, ms_tmp, key_tmp, mouse_tmp, guide_tmp, sems,
):
    heads, _, hd = own_ref.shape
    frames = kb_tmp.shape[0]
    head = pl.ds(pl.multiple_of(head_ref[0] * hd, hd), hd)
    ids = [
        pltpu.make_async_copy(kb_ref, kb_tmp, sems.at[0]),
        pltpu.make_async_copy(ms_ref, ms_tmp, sems.at[1]),
    ]
    picks = [
        pltpu.make_async_copy(guide_ref, guide_tmp, sems.at[2]),
        pltpu.make_async_copy(w_ref.at[:, head], w_tmp, sems.at[3]),
    ]
    for copy in ids + picks:
        copy.start()
    count = share_ref.shape[0]
    before, after = lax.rem(at_ref[0] + (count - 1), count), lax.rem(at_ref[0] + 1, count)
    earlier = share_ref[pl.ds(before, 1), heads + 1, 0:rows, :].reshape(rows, hd)
    later = share_ref[pl.ds(after, 1), heads, 0:rows, :].reshape(rows, hd)
    query = own_ref[:, 0:rows, :].reshape(heads * rows, hd)
    query_ref[0:rows, :] = earlier
    query_ref[rows : rows + heads * rows, :] = query
    query_ref[rows + heads * rows :, :] = later
    for f in range(frames):
        at = 4 + 2 * f
        picks += [
            (key_ref, kb_tmp, key_tmp, f, sems.at[at]),
            (mouse_ref, ms_tmp, mouse_tmp, f, sems.at[at + 1]),
        ]

    def fetch():
        for copy in ids:
            copy.wait()
        for n in range(2, len(picks)):
            table, chosen, rows_tmp, f, sem = picks[n]
            picks[n] = pltpu.make_async_copy(table.at[chosen[f], :, head], rows_tmp.at[f], sem)
            picks[n].start()

    share_body(rows, sets, heads, query_ref[...], share_ref, sum_ref, top_ref, total_ref, fetch)
    for copy in picks:
        copy.wait()
    rows_key = key_tmp[...].astype(F32)
    rows_mouse = mouse_tmp[...].astype(F32)
    bias_key, bias_mouse = rows_key[:, 0, :], rows_mouse[:, 0, :]
    bias = [bias_key + bias_mouse, bias_mouse, bias_key, jnp.zeros_like(bias_key)]
    bias_ref[...] = jnp.concatenate(bias, axis=0).astype(BF)
    terms = jnp.concatenate([rows_key[:, 1, :], rows_mouse[:, 1, :]], axis=0).astype(BF)
    term_ref[...] = dot(terms, w_tmp[...], ((1,), (1,)))
    for b in range(line_ref.shape[0]):
        line_ref[b : b + 1, :] = jnp.full((1, hd), guide_tmp[b], F32)


def share_shapes(share, heads, rows, sets, outs):
    tokens = (heads + 2) * rows
    frames = share.shape[0] * heads // sets
    shapes = [
        jax.ShapeDtypeStruct((frames, outs, tokens), F32),
        jax.ShapeDtypeStruct((frames, tokens), F32),
        jax.ShapeDtypeStruct((frames, tokens), F32),
    ]
    keys = frames * sets * rows
    cost = pl.CostEstimate(
        flops=2 * tokens * keys * (HEAD_DIM + outs),
        transcendentals=tokens * keys,
        bytes_accessed=1 << 20,
    )
    return tokens, shapes, cost


def own_share_attention(
    place, head, own, share, weight_t, keyboard, mouse, key_table, mouse_table, guidance, rows, sets
):
    outs = weight_t.shape[0]
    frames = keyboard.shape[0]
    tokens, shapes, cost = share_shapes(share, own.shape[0], rows, sets, outs)
    arrays = (weight_t, keyboard, mouse, key_table, mouse_table, guidance)
    return pl.pallas_call(
        functools.partial(own_share_kernel, rows, sets),
        in_specs=[SMEM, SMEM, VMEM, VMEM] + [HBM] * len(arrays),
        out_specs=[VMEM] * 7,
        out_shape=[jax.ShapeDtypeStruct((tokens, HEAD_DIM), BF)]
        + shapes
        + [
            jax.ShapeDtypeStruct((4 * frames, HEAD_DIM), BF),
            jax.ShapeDtypeStruct((2 * frames, outs), F32),
            jax.ShapeDtypeStruct((guidance.shape[0], HEAD_DIM), F32),
        ],
        scratch_shapes=[pltpu.VMEM((outs, HEAD_DIM), BF)]
        + [pltpu.SMEM((frames,), jnp.int32)] * 2
        + [pltpu.VMEM((frames, 2, HEAD_DIM), BF)] * 2
        + [pltpu.SMEM(guidance.shape, F32), pltpu.SemaphoreType.DMA((4 + 2 * frames,))],
        cost_estimate=cost,
        name="own_share",
        compiler_params=GRANT,
    )(place[None], head[None], own, share, *(in_hbm(a) for a in arrays))


def guide_kernel(rows, guide_ref, query_ref, bias_ref, term_ref, *refs):
    shares, out_ref = refs[:-1], refs[-1]
    sum_refs, top_refs, total_refs = shares[0::3], shares[1::3], shares[2::3]
    heads = out_ref.shape[0]
    half = rows // 2
    count = top_refs[0].shape[0]
    shift = dot(bias_ref[...], query_ref[...], ((1,), (1,)))
    tops = [r[...] for r in top_refs]
    totals = [r[...] for r in total_refs]
    mixes = [None] * len(tops)
    by_key, by_mouse = None, None
    for b in range(4):
        heights = [(top + shift[b * count : (b + 1) * count]) * TO_EXP2 for top in tops]
        peak = functools.reduce(jnp.maximum, heights)
        peak = jnp.max(peak, axis=0, keepdims=True)
        factors = [jnp.exp2(height - peak) for height in heights]
        loads = functools.reduce(jnp.add, [f * t for f, t in zip(factors, totals)])
        scale = guide_ref[b : b + 1, 0:1] / jnp.sum(loads, axis=0, keepdims=True)
        parts = [f * scale for f in factors]
        mixes = [p if m is None else m + p for m, p in zip(mixes, parts)]
        loads = loads * scale
        if b % 2 == 0:
            by_key = loads if by_key is None else by_key + loads
        if b < 2:
            by_mouse = loads if by_mouse is None else by_mouse + loads
    loads = jnp.concatenate([by_key, by_mouse], axis=0)
    result = dot(term_ref[...], loads, ((0,), (0,)), precision=lax.Precision.HIGHEST)
    for mix, sum_ref in zip(mixes, sum_refs):
        for frame in range(count):
            result = result + mix[frame : frame + 1, :] * sum_ref[frame]
    by_token = jnp.transpose(result).reshape(heads + 2, 2, half, -1)
    packed = jnp.concatenate([by_token[:, 0], by_token[:, 1]], axis=2).astype(BF)
    for side in range(3):
        out_ref[:, side * half : (side + 1) * half, :] = packed[side : side + heads]


def other_share_kernel(
    rows, sets, query_ref, share_ref, line_ref, bias_ref, term_ref,
    sum_ref, top_ref, total_ref, out_ref, sum_tmp, top_tmp, total_tmp,
):
    heads = out_ref.shape[0]
    share_body(rows, sets, heads, query_ref[...], share_ref, sum_tmp, top_tmp, total_tmp)
    shares = (sum_ref, top_ref, total_ref, sum_tmp, top_tmp, total_tmp)
    guide_kernel(rows, line_ref, query_ref, bias_ref, term_ref, *shares, out_ref)


def other_share_and_guide(query, share, lines, bias, term, first, rows, sets, outs):
    heads = query.shape[0] // rows - 2
    _, shapes, cost = share_shapes(share, heads, rows, sets, outs)
    return pl.pallas_call(
        functools.partial(other_share_kernel, rows, sets),
        in_specs=[VMEM] * 8,
        out_specs=VMEM,
        out_shape=jax.ShapeDtypeStruct((heads, 3 * (rows // 2), 2 * outs), BF),
        scratch_shapes=[pltpu.VMEM(a.shape, a.dtype) for a in shapes],
        cost_estimate=cost,
        name="other_share",
        compiler_params=GRANT,
    )(query, share, lines, bias, term, *first)


def decode_kernel(
    flag_ref, mine_ref, other_ref, noisy_ref, conv_in_ref, gain_ref, conv_out_ref,
    velocity_out, colours_out, velocity_ref, out_ref, sems,
):
    outs = velocity_ref.shape[1]
    lat = outs // 4
    tokens = velocity_ref.shape[0]
    quarter = tokens // 4
    first, last = flag_ref[0:1, 0:1] > 0.5, flag_ref[1:2, 0:1] > 0.5
    low_core = flag_ref[2:3, :] > 0.5
    left, right = [], []
    for side in range(3):
        place = slice(side * quarter, (side + 1) * quarter)
        here, there = mine_ref[place, :], other_ref[place, :]
        both = [jnp.where(low_core, here, there), jnp.where(low_core, there, here)]
        blocks = []
        for n, velocity in enumerate(both):
            stepped = noisy_ref[side, n * quarter : (n + 1) * quarter, :] - step_size * velocity
            blocks += [stepped[:, :outs], stepped[:, outs:]]
            if side == 1:
                at = 2 * n * quarter
                velocity_ref[at : at + quarter, :] = velocity[:, :outs]
                velocity_ref[at + quarter : at + 2 * quarter, :] = velocity[:, outs:]
        block = jnp.concatenate(blocks, axis=0).astype(BF).astype(F32)
        if side == 1:
            velocity_copy = pltpu.make_async_copy(velocity_ref, velocity_out, sems.at[0])
            velocity_copy.start()
        else:
            block = jnp.where(first if side == 0 else last, 0.0, block)
        edge = jnp.zeros_like(block[:1])
        earlier = jnp.concatenate([edge, block[:-1]], axis=0)
        later = jnp.concatenate([block[1:], edge], axis=0)
        for dy in range(2):
            at = 2 * lat * dy
            here = block[:, at : at + 2 * lat]
            left.append(jnp.concatenate([earlier[:, at + lat : at + 2 * lat], here], axis=1))
            right.append(jnp.concatenate([here, later[:, at : at + lat]], axis=1))
    height = 4 * tokens
    row = lax.broadcasted_iota(jnp.int32, (height, 1), 0) // tokens
    keep = jnp.where((row == 0) & first | (row == 3) & last, 0.0, 1.0)
    taps = []
    for windows in (left, right):
        stack = jnp.concatenate(windows, axis=0).astype(BF)
        features = dot(stack[:height], conv_in_ref[0], ((1,), (0,)))
        for a in range(1, 3):
            part = stack[a * tokens : a * tokens + height]
            features = features + dot(part, conv_in_ref[a], ((1,), (0,)))
        power = jnp.mean(features * features, axis=1, keepdims=True)
        scaled = features * lax.rsqrt(power + norm_eps) * gain_ref[...]
        normed = scaled / (1.0 + jnp.exp(-scaled)) * keep
        taps.append(dot(conv_out_ref[...], normed.astype(BF), ((1,), (1,))))
    even, odd = taps
    step = even.shape[0] // 3
    lane = lax.broadcasted_iota(jnp.int32, (step, height), 1) % tokens
    before = jnp.where(lane == 0, 0.0, pltpu.roll(odd[:step], 1, 1))
    after = jnp.where(lane == tokens - 1, 0.0, pltpu.roll(even[2 * step :], height - 1, 1))
    columns = [
        before + even[step : 2 * step] + odd[2 * step :],
        even[:step] + odd[step : 2 * step] + after,
    ]
    source = lax.broadcasted_iota(jnp.int32, (height, height), 0)
    target = lax.broadcasted_iota(jnp.int32, (height, height), 1)
    colours = None
    for dx, column in enumerate(columns):
        moved = column[0:3]
        for a in range(1, 3):
            moved = moved + pltpu.roll(column[3 * a : 3 * a + 3], height - a * tokens, 1)
        chosen = jnp.where(target == 2 * source + dx, 1.0, 0.0)
        placed = dot(moved, chosen, ((1,), (0,)), precision=lax.Precision.HIGHEST)
        colours = placed if colours is None else colours + placed
    out_ref[:, 0, :] = colours[:, : 2 * tokens]
    out_ref[:, 1, :] = colours[:, 2 * tokens :]
    colours_copy = pltpu.make_async_copy(out_ref, colours_out, sems.at[1])
    colours_copy.start()
    velocity_copy.wait()
    colours_copy.wait()


def decode(flags, mine, other, noisy, conv_in, gain, conv_out):
    tokens, outs = 2 * noisy.shape[1], noisy.shape[2] // 2
    return pl.pallas_call(
        decode_kernel,
        in_specs=[VMEM] * 7,
        out_specs=[pl.BlockSpec(memory_space=pltpu.HBM)] * 2,
        out_shape=[
            jax.ShapeDtypeStruct((tokens, outs), F32),
            jax.ShapeDtypeStruct((3, 2, 2 * tokens), F32),
        ],
        scratch_shapes=[
            pltpu.VMEM((tokens, outs), F32),
            pltpu.VMEM((3, 2, 2 * tokens), F32),
            pltpu.SemaphoreType.DMA((2,)),
        ],
        name="decode",
        compiler_params=GRANT,
    )(flags, mine, other, noisy, conv_in, gain, conv_out)


def shards(
    queries,
    keys,
    values,
    keyboard,
    mouse,
    key_table,
    mouse_table,
    guidance,
    out_weight,
    latent,
    conv_in,
    gain,
    conv_out,
):
    wide, narrow, sets = lax.axis_size("xh"), lax.axis_size("xl"), lax.axis_size("z")
    xh, xl, z = lax.axis_index("xh"), lax.axis_index("xl"), lax.axis_index("z")
    cores = lax.axis_size("branch")
    core = lax.axis_index("branch")
    outs = out_weight.shape[1]
    assert keyboard.shape[0] == wide * narrow and cores == 2
    rows = queries.shape[0] // cores
    swap = [(0, 1), (1, 0)]

    weight_t = out_weight.T
    packed = pack(core, queries, keys, values, weight_t, rows)
    own = lax.all_to_all(packed, ("xh", "z"), 0, 0, tiled=True)
    moving = jnp.concatenate(
        [own[:, rows:], own[:1, : rows + rows // 2], own[-1:, : rows + rows // 2]], axis=0
    )
    share = lax.all_gather(moving, "xl")
    other_share = lax.ppermute(share, "branch", swap)
    query, *first, bias, term, lines = own_share_attention(
        xl, xh * sets + z, own, share, weight_t,
        keyboard, mouse, key_table, mouse_table, guidance, rows, sets,
    )
    part = other_share_and_guide(query, other_share, lines, bias, term, first, rows, sets, outs)
    part, latent, conv_out, gain = lax.optimization_barrier((part, latent, conv_out, gain))
    returned = lax.all_to_all(part, ("xh", "z"), 0, 0, tiled=True)

    count = wide * narrow * sets
    places = ("xl", "xh", "z")
    index = (xl * wide + xh) * sets + z
    line = lax.broadcasted_iota(jnp.int32, (8, HEAD_DIM), 0)
    flags = (line == 0) & (index == 0) | (line == 1) & (index == count - 1) | (line == 2) & (core == 0)
    flags = flags.astype(F32)
    taps_in = conv_in.reshape(conv_in.shape[0], -1, conv_in.shape[3])
    taps_out = conv_out.transpose(1, 0, 3, 2).reshape(3, -1, conv_out.shape[2])
    taps_out = jnp.pad(taps_out, ((0, 0), (0, 16 - taps_out.shape[1]), (0, 0)))
    taps_out = taps_out.reshape(-1, conv_out.shape[2])
    noisy = latent.reshape(2, 2, -1, outs).transpose(0, 2, 1, 3).reshape(-1, 2 * outs)
    before = lax.ppermute(noisy, places, [(i, i + 1) for i in range(count - 1)])
    after = lax.ppermute(noisy, places, [(i + 1, i) for i in range(count - 1)])
    noisy = jnp.stack([before, noisy, after])
    mine = jnp.sum(returned.astype(F32), axis=0)
    mine, noisy, taps_out, gain, flags = lax.optimization_barrier(
        (mine, noisy, taps_out, gain[None], flags)
    )
    other = lax.ppermute(mine, "branch", swap)
    return tuple(decode(flags, mine, other, noisy, taps_in, gain, taps_out))


def solution(mesh):
    cores = mesh.shape["branch"]
    tok = mesh.shape["tok"]

    def run(*arrays):
        heads = arrays[0].shape[1] // HEAD_DIM
        sets = heads // cores
        fine = Mesh(
            mesh.devices.reshape(mesh.shape["groups"], cores, tok // heads, cores, sets),
            ("groups", "branch", "xl", "xh", "z"),
        )
        tokens = P(("groups", "xl", "xh", "z"), None)
        placed = (
            tokens,
            tokens,
            tokens,
            P("groups"),
            P("groups"),
            P(),
            P(),
            P(),
            P(),
            tokens,
            P(),
            P(),
            P(),
        )
        return jax.shard_map(
            shards,
            mesh=fine,
            in_specs=placed,
            out_specs=(tokens, P(None, ("groups", "xl", "xh", "z"), None)),
            check_vma=False,
        )(*arrays)

    return run
```
